32 devices in a mesh: parts: 2 (over y), expert: 4 (over z), tensor: 4 (over x, core).
Axes of the slice: x: 2, y: 2, z: 4, core: 2. Of those that a mesh axis runs over, the one named last changes fastest.
Arguments:
- mamba_input: bfloat16 [128, 4096], P(('parts', 'expert'), 'tensor'), parts along dimension 0, may hold values from -5 to 5
- mamba_gate: bfloat16 [128, 4096], P(('parts', 'expert'), 'tensor'), parts along dimension 0, may hold values from -5 to 5
- conv_state: bfloat16 [128, 3, 4096], P(('parts', 'expert'), None, 'tensor'), parts along dimension 0, may hold values from -5 to 5
- scan_state: float32 [128, 16, 4096], P(('parts', 'expert'), None, 'tensor'), parts along dimension 0, may hold values from -6 to 6
- conv_weight: float32 [4, 4096], P(None, 'tensor'), may hold values from -3 to 3
- conv_bias: float32 [4096], P('tensor'), may hold values from -0.5 to 0.5
- state_proj: bfloat16 [288, 4096], P(None, 'tensor'), may hold values from -0.09375 to 0.09375
- step_proj: bfloat16 [256, 4096], P(None, 'tensor'), may hold values from -0.375 to 0.375
- step_bias: float32 [4096], P('tensor'), may hold values from -4.5 to -1
- decay_log: float32 [16, 4096], P(None, 'tensor'), may hold values from 0 to 2.8
- skip_gain: float32 [4096], P('tensor'), may hold values from 0.5 to 2
- queries: bfloat16 [128, 32, 128], P(('parts', 'expert'), 'tensor'), parts along dimension 0, may hold values from -48 to 48
- new_entry: bfloat16 [128, 8, 256], P(('parts', 'expert'), 'tensor'), parts along dimension 0, may hold values from -4 to 4
- past_entries: bfloat16 [128, 8, 128, 256], P(('parts', 'expert'), 'tensor'), parts along dimension 0, may hold values from -4 to 4
- lengths: int32 [128], P(('parts', 'expert')), parts along dimension 0, may hold values from 2 to 128, as said below
- expert_input: bfloat16 [128, 2048], P(('parts', 'expert'), 'tensor'), parts along dimension 0, may hold values from -5 to 5
- routes: int32 [128, 2], P(('parts', 'expert')), parts along dimension 0, may hold values from 0 to 7, as said below
- slots: int32 [128, 2], P(('parts', 'expert')), parts along dimension 0, may hold values from 0 to 7, as said below
- gates: float32 [128, 2], P(('parts', 'expert')), parts along dimension 0, may hold values from 0.1 to 1
- inner_weights: bfloat16 [8, 2, 8192, 2048], P('expert', None, 'tensor'), may hold values from -0.125 to 0.125
- outer_weights: bfloat16 [8, 8192, 2048], P('expert', 'tensor'), may hold values from -0.09375 to 0.09375
Outputs:
- mamba_out: bfloat16 [128, 4096], P(('parts', 'expert'), 'tensor'), parts along dimension 0
- next_state: float32 [128, 16, 4096], P(('parts', 'expert'), None, 'tensor'), parts along dimension 0
- attention_out: bfloat16 [128, 4096], P(('parts', 'expert'), 'tensor'), parts along dimension 0
- expert_out: bfloat16 [128, 2048], P(('parts', 'expert'), 'tensor'), parts along dimension 0
The draws below stay inside these ranges and needn't reach their ends.
There are 2 independent parts, one for each index of `parts`. The reference program is written for one: setup_inputs(seed, part) draws one part's arguments, and reference() takes and returns one part's arrays. A program takes and returns all parts, laid end to end along the dimension named above; an argument that names none is the same for every part. Nothing has to cross between parts.
Inputs may be any that keep to these rules, and one draw needn't show every extreme that they name: `routes`: A row names 2 different experts. Within the 16 rows of one device (aligned blocks) no expert is named more than 8 times, and one expert, the same in all blocks, is named exactly 8 times in every block. slots[t, k] numbers the rows of t's block that name expert routes[t, k]: within a block the slots of one expert are distinct. `lengths`: every block of 16 sequences holds one of length 128.
All inputs are finite; a program needn't handle non-finite values.
Results may differ from the reference program's by a relative error of at most 0.006.
Values may be sent and summed in bfloat16 or wider, within the bound.
No kernel may reach another device: no remote copies, remote signals or barrier semaphores. Data moves between devices by JAX's collectives and lax.ppermute only.
A program may use at most 128 MiB of HBM per device.

```python
import jax
import jax.numpy as jnp
from jax import lax

D = 2048
FF = 8192
EXPERTS = 8
TOP = 2
INNER = 4096
NS = 16
R = 256
CONV = 4
QH = 32
KVH = 8
HD = 128
B_DEV = 16
CACHE = 128
SEQS = 64
REP = 1
ROWS = 8
FFR = 8192
CAP = 8
PROJ = 288


def route_table(key):
    blocks = SEQS // B_DEV
    capacity = max(2, 4 * B_DEV // EXPERTS)
    hot_expert = jax.random.randint(jax.random.fold_in(key, 11), (), 0, EXPERTS).astype(jnp.int32)
    cell_count = (EXPERTS - 1) * capacity

    def one_block(block_key):
        first_key, second_key = jax.random.split(block_key)
        ranked = jax.random.permutation(first_key, cell_count)
        taken_cells = (ranked < 2 * B_DEV - capacity).astype(jnp.int32)
        counts = jnp.concatenate([jnp.full((1,), capacity, jnp.int32), jnp.sum(taken_cells.reshape(EXPERTS - 1, capacity), axis=1)])
        others = jnp.arange(EXPERTS - 1, dtype=jnp.int32)
        others = others + (others >= hot_expert).astype(jnp.int32)
        expert_order = jnp.concatenate([hot_expert[None], others])
        upper_edge = jnp.cumsum(counts)
        lower_edge = upper_edge - counts
        positions = jnp.arange(2 * B_DEV, dtype=jnp.int32)
        run_index = jnp.sum((upper_edge[None, :] <= positions[:, None]).astype(jnp.int32), axis=1)
        chosen = expert_order[run_index]
        slot_pos = positions - lower_edge[run_index]
        pair_experts = jnp.stack([chosen[:B_DEV], chosen[B_DEV:]], axis=1)
        pair_slots = jnp.stack([slot_pos[:B_DEV], slot_pos[B_DEV:]], axis=1)
        shuffle = jax.random.permutation(second_key, B_DEV)
        return (pair_experts[shuffle], pair_slots[shuffle])
    block_keys = jax.random.split(jax.random.fold_in(key, 12), blocks)
    experts_drawn, slots_drawn = jax.vmap(one_block)(block_keys)
    return (experts_drawn.reshape(SEQS, 2).astype(jnp.int32), slots_drawn.reshape(SEQS, 2).astype(jnp.int32))


def draw_routes(key, part):
    return route_table(key)[0]


def draw_slots(key, part):
    return route_table(key)[1]


def draw_lengths(key, part):
    base_len = jax.random.randint(jax.random.fold_in(key, 21), (SEQS,), 2, CACHE + 1)
    full_pick = jax.random.randint(jax.random.fold_in(key, 22), (SEQS // B_DEV,), 0, B_DEV)
    full_mask = (jnp.arange(B_DEV, dtype=jnp.int32)[None, :] == full_pick[:, None]).reshape(SEQS)
    return jnp.where(full_mask, CACHE, base_len).astype(jnp.int32)


def attention_tables(key):
    cache_shape = (SEQS, KVH, CACHE, 2 * HD)
    entries = jnp.clip(jax.random.normal(jax.random.fold_in(key, 31), cache_shape, jnp.float32), -4.0, 4.0)
    query_rows = jnp.clip(jax.random.normal(jax.random.fold_in(key, 32), (SEQS, QH, HD), jnp.float32), -4.0, 4.0)
    return (query_rows, entries)


def draw_queries(key, part):
    return attention_tables(key)[0].astype(jnp.bfloat16)


def draw_past_entries(key, part):
    return attention_tables(key)[1].astype(jnp.bfloat16)


def strengthened(drawn, rng, source, target, shards_of, factor):
    owner, partner = [(jnp.arange(drawn.shape[axis_at]) // (drawn.shape[axis_at] // shards_of)).reshape([-1 if axis == axis_at else 1 for axis in range(drawn.ndim)]) for axis_at in (source, target)]
    chosen = jax.random.permutation(rng, shards_of)[partner]
    strong = (owner == chosen) | (owner == (partner + shards_of // 2) % shards_of)
    return jnp.where(strong, factor * drawn, drawn)


def shard_levels(stream_key, extent, cuts, least, top_value):
    gain = 1.0
    for dim, parts in cuts:
        draws = jax.random.uniform(jax.random.fold_in(jax.random.fold_in(stream_key, 6), dim), (parts,), jnp.float32, least / len(cuts), top_value / len(cuts))
        gain = gain * jnp.repeat(jnp.exp(draws), extent[dim] // parts).reshape((-1,) + (1,) * (len(extent) - 1 - dim))
    return gain


def normal_values(key, extent, spread, limit, cuts=(), kind=jnp.bfloat16):
    drawn = jax.random.normal(key, extent, jnp.float32) * spread
    if len(cuts) > 0:
        drawn = shard_levels(key, extent, cuts, -0.22, 0.18) * drawn
    return jnp.clip(drawn, min=-limit, max=limit).astype(kind)


def gaussian_with(stream_key, dims, width, most, cuts, heavy, held_as=jnp.bfloat16):
    drawn = width * jax.random.normal(stream_key, dims, jnp.float32)
    if cuts:
        drawn = drawn * shard_levels(stream_key, dims, cuts, -0.22, 0.18)
    return jnp.clip(strengthened(drawn, jax.random.fold_in(stream_key, 3), *heavy), -most, most).astype(held_as)


def setup_inputs(seed: int = 0, part: int = 0) -> dict:
    splits = jax.random.split(jax.random.key(seed), 22)
    part_splits = jax.random.split(jax.random.fold_in(splits[21], part), 22)
    mamba_input = normal_values(part_splits[0], (SEQS, INNER), 1.0, 5.0, ((0, 4), (1, 4)))
    mamba_gate = normal_values(part_splits[1], (SEQS, INNER), 1.0, 5.0, ((0, 4), (1, 4)))
    conv_state = normal_values(part_splits[2], (SEQS, CONV - 1, INNER), 1.0, 5.0, ((0, 4), (2, 4)))
    scan_state = normal_values(part_splits[3], (SEQS, NS, INNER), 1.0, 6.0, ((0, 4), (2, 4)), jnp.float32)
    conv_weight = normal_values(splits[4], (CONV, INNER), CONV ** -0.5, 3.0, ((1, 4),), jnp.float32)
    conv_bias = jnp.clip(jax.random.uniform(splits[5], (INNER,), jnp.float32, -0.5, 0.5) * shard_levels(splits[5], (INNER,), ((0, 4),), -0.4, 0.0), -0.5, 0.5)
    state_proj = normal_values(splits[6], (PROJ, INNER), INNER ** -0.5, 0.09375, ((1, 4),))
    step_proj = normal_values(splits[7], (R, INNER), R ** -0.5, 0.375, ((1, 4),))
    step_bias = jnp.clip(-4.5 + 3.5 * jax.random.uniform(splits[8], (INNER,), jnp.float32) ** shard_levels(splits[8], (INNER,), ((0, 4),), -0.2, 0.2), -4.5, -1.0)
    decay_log = jnp.clip(2.8 * jax.random.uniform(splits[9], (NS, INNER), jnp.float32) ** shard_levels(splits[9], (NS, INNER), ((1, 4),), -0.2, 0.2), 0.0, 2.8)
    skip_gain = jnp.clip(0.5 + 1.5 * jax.random.uniform(splits[10], (INNER,), jnp.float32) ** shard_levels(splits[10], (INNER,), ((0, 4),), -0.2, 0.2), 0.5, 2.0)
    queries = draw_queries(jax.random.fold_in(jax.random.fold_in(splits[21], part), 71), part)
    new_entry = normal_values(part_splits[12], (SEQS, KVH, 2 * HD), 1.0, 4.0, ((0, 4), (1, 4)))
    past_entries = draw_past_entries(jax.random.fold_in(jax.random.fold_in(splits[21], part), 71), part)
    lengths = draw_lengths(jax.random.fold_in(jax.random.fold_in(splits[21], part), 71), part)
    expert_input = normal_values(part_splits[15], (SEQS, D), 1.0, 5.0, ((0, 4), (1, 4)))
    routes = draw_routes(jax.random.fold_in(jax.random.fold_in(splits[21], part), 71), part)
    slots = draw_slots(jax.random.fold_in(jax.random.fold_in(splits[21], part), 71), part)
    gates = jnp.clip(0.1 + 0.9 * jax.random.uniform(part_splits[18], (SEQS, TOP), jnp.float32) ** shard_levels(part_splits[18], (SEQS, TOP), ((0, 4),), -0.2, 0.2), 0.1, 1.0)
    inner_weights = normal_values(splits[19], (ROWS, 2, FFR, D), D ** -0.5, 0.125, ((0, 4), (2, 4)))
    outer_weights = gaussian_with(splits[20], (ROWS, FFR, D), FF ** -0.5, 0.09375, ((0, 4), (1, 4)), (1, 2, 4, 2.0))
    return dict(mamba_input=mamba_input, mamba_gate=mamba_gate, conv_state=conv_state, scan_state=scan_state, conv_weight=conv_weight, conv_bias=conv_bias, state_proj=state_proj, step_proj=step_proj, step_bias=step_bias, decay_log=decay_log, skip_gain=skip_gain, queries=queries, new_entry=new_entry, past_entries=past_entries, lengths=lengths, expert_input=expert_input, routes=routes, slots=slots, gates=gates, inner_weights=inner_weights, outer_weights=outer_weights)


def mamba_step(mamba_input, mamba_gate, conv_state, scan_state, conv_weight, conv_bias, state_proj, step_proj, step_bias, decay_log, skip_gain):
    window = jnp.concatenate([conv_state.astype(jnp.float32), mamba_input.astype(jnp.float32)[:, None, :]], axis=1)
    conv_act = jax.nn.silu(jnp.sum(window * conv_weight[None], axis=1) + conv_bias)
    mixing = lax.dot_general(conv_act.astype(jnp.bfloat16), state_proj, (((1,), (1,)), ((), ())), preferred_element_type=jnp.float32)
    low_rank = step_proj.shape[0]
    states = decay_log.shape[0]
    step_size = jax.nn.softplus(jnp.dot(mixing[:, :low_rank].astype(jnp.bfloat16), step_proj, preferred_element_type=jnp.float32) + step_bias)
    in_coef = mixing[:, low_rank:low_rank + states]
    out_coef = mixing[:, low_rank + states:]
    decay_rate = jnp.exp(-step_size[:, None, :] * jnp.exp(decay_log)[None])
    next_state = decay_rate * scan_state + (step_size * conv_act)[:, None, :] * in_coef[:, :, None]
    mixed_out = jnp.sum(next_state * out_coef[:, :, None], axis=1) + skip_gain * conv_act
    return (mixed_out * jax.nn.silu(mamba_gate.astype(jnp.float32))).astype(jnp.bfloat16), next_state


def attend(queries, new_entry, past_entries, lengths):
    seq_count, head_count, head_size = queries.shape
    groups = past_entries.shape[1]
    per_group = head_count // groups
    positions = past_entries.shape[2]
    scaling = head_size ** -0.5
    query_rows = queries.astype(jnp.float32).reshape(seq_count, groups, per_group, head_size)
    cache_keys = past_entries[..., :head_size].astype(jnp.float32)
    cache_values = past_entries[..., head_size:].astype(jnp.float32)
    scores = jnp.einsum("sgqd,sgld->sgql", query_rows, cache_keys) * scaling
    own_score = jnp.einsum("sgqd,sgd->sgq", query_rows, new_entry[..., :head_size].astype(jnp.float32)) * scaling
    live_mask = jnp.arange(positions, dtype=jnp.int32)[None, :] < lengths[:, None]
    scores = jnp.where(live_mask[:, None, None, :], scores, -jnp.inf)
    highest = jnp.maximum(jnp.max(scores, axis=3), own_score)
    weights = jnp.exp(scores - highest[..., None])
    own_weight = jnp.exp(own_score - highest)
    denominator = jnp.sum(weights, axis=3) + own_weight
    weights_low = (weights / denominator[..., None]).astype(jnp.bfloat16)
    own_low = (own_weight / denominator).astype(jnp.bfloat16)
    mixed_out = jnp.einsum("sgql,sgld->sgqd", weights_low.astype(jnp.float32), cache_values)
    mixed_out = mixed_out + own_low.astype(jnp.float32)[..., None] * new_entry[..., head_size:].astype(jnp.float32)[:, :, None, :]
    return mixed_out.reshape(seq_count, head_count * head_size).astype(jnp.bfloat16)


def expert_layer(expert_input, routes, slots, gates, inner_weights, outer_weights):
    blocks = SEQS // B_DEV
    source = jnp.broadcast_to((jnp.arange(SEQS, dtype=jnp.int32) // B_DEV)[:, None], routes.shape)
    buffer = jnp.zeros((EXPERTS, blocks, CAP, D), jnp.bfloat16)
    buffer = buffer.at[routes, source, slots].set(jnp.broadcast_to(expert_input[:, None, :], (SEQS, TOP, D)))

    def one_expert(operands):
        token_rows, inner_w, outer_w = operands
        gate_w = inner_w[:, 0].reshape(FF, D)
        up_w = inner_w[:, 1].reshape(FF, D)
        gate_val = lax.dot_general(token_rows, gate_w, (((1,), (1,)), ((), ())), preferred_element_type=jnp.float32)
        up_val = lax.dot_general(token_rows, up_w, (((1,), (1,)), ((), ())), preferred_element_type=jnp.float32)
        hidden = (jax.nn.silu(gate_val) * up_val).astype(jnp.bfloat16)
        return jnp.dot(hidden, outer_w.reshape(FF, D), preferred_element_type=jnp.float32)

    results = lax.map(one_expert, (buffer.reshape(EXPERTS, blocks * CAP, D), inner_weights.reshape(EXPERTS, REP, 2, FFR, D), outer_weights.reshape(EXPERTS, REP, FFR, D)))
    results = results.reshape(EXPERTS, blocks, CAP, D)
    picked = results[routes, source, slots]
    return jnp.sum(gates[:, :, None] * picked, axis=1).astype(jnp.bfloat16)


def reference(mamba_input, mamba_gate, conv_state, scan_state, conv_weight, conv_bias, state_proj, step_proj, step_bias, decay_log, skip_gain, queries, new_entry, past_entries, lengths, expert_input, routes, slots, gates, inner_weights, outer_weights):
    mamba_out, next_state = mamba_step(mamba_input, mamba_gate, conv_state, scan_state, conv_weight, conv_bias, state_proj, step_proj, step_bias, decay_log, skip_gain)
    attention_out = attend(queries, new_entry, past_entries, lengths)
    expert_out = expert_layer(expert_input, routes, slots, gates, inner_weights, outer_weights)
    return (mamba_out, next_state, attention_out, expert_out)
```

```python
import functools

import jax
import jax.numpy as jnp
from jax import lax
from jax.experimental import pallas as pl
from jax.experimental.pallas import tpu as pltpu
from jax.sharding import PartitionSpec as P

EXPERTS = 8
LANES = 128
F32 = jnp.float32
BF16 = jnp.bfloat16

HBM_SPEC = pl.BlockSpec(memory_space=pl.ANY)
VMEM_SPEC = pl.BlockSpec(memory_space=pltpu.VMEM)


def silu(v):
    return v / (1.0 + jnp.exp(-v))


def split_bf16(v):
    high = v.astype(BF16)
    return high, (v - high.astype(F32)).astype(BF16)


def partner(index, step, count):
    if count & (count - 1) == 0:
        return index ^ step
    return (index + step) % count


def returner(index, step, count):
    if count & (count - 1) == 0:
        return index ^ step
    return (index - step) % count


def exchange(blocks, axis, back=False):
    count = lax.axis_size(axis)
    rule = returner if back else partner
    out = {0: blocks[0]}
    for step in range(count - 1, 0, -1):
        pairs = [(i, rule(i, step, count)) for i in range(count)]
        out[step] = lax.ppermute(blocks[step], axis, pairs)
    return [out[step] for step in range(count)]


def front_kernel(
    width,
    past_hbm, queries_hbm, entry_hbm, lengths_ref, state_hbm, input_hbm,
    taps_hbm, bias_hbm, proj_hbm,
    attn_hbm, act_ref, mix_ref,
    past, queries, entry, state, inputs, taps, bias, proj, heads, attn, sems,
):
    seqs, head_count, size = queries.shape
    groups = past.shape[1]
    per_group = head_count // groups
    positions = past.shape[2]
    parts = 4 if seqs % 4 == 0 else 1
    part = seqs // parts
    small = [
        pltpu.make_async_copy(src, dst, sems.at[n])
        for n, (src, dst) in enumerate((
            (queries_hbm, queries), (entry_hbm, entry), (state_hbm, state),
            (input_hbm, inputs), (taps_hbm, taps), (bias_hbm, bias), (proj_hbm, proj),
        ))
    ]
    large = [
        pltpu.make_async_copy(
            past_hbm.at[pl.ds(n * part, part)], past.at[pl.ds(n * part, part)],
            sems.at[len(small) + n],
        )
        for n in range(parts)
    ]
    for copy in small + large:
        copy.start()
    for copy in small:
        copy.wait()

    total = bias[...]
    for k in range(taps.shape[0] - 1):
        total = total + state[:, k, :].astype(F32) * taps[k : k + 1, :]
    total = total + inputs[...].astype(F32) * taps[taps.shape[0] - 1 :, :]
    act = silu(total)
    act_ref[...] = act
    mix = lax.dot_general(
        act.astype(BF16), proj[...], (((1,), (1,)), ((), ())), preferred_element_type=F32
    )
    outputs = mix.shape[1]
    spans = -(-outputs // width)
    row = 0
    for piece in split_bf16(mix):
        for span in range(spans):
            cut = piece[:, span * width : min(outputs, (span + 1) * width)]
            if cut.shape[1] < width:
                cut = jnp.concatenate(
                    [cut.astype(F32), jnp.zeros((seqs, width - cut.shape[1]), F32)], axis=1
                ).astype(BF16)
            mix_ref[row : row + seqs, :] = cut
            row += seqs

    scaling = size ** (-0.5)
    rows = lax.broadcasted_iota(jnp.int32, (head_count, positions), 0) // per_group
    owner = lax.broadcasted_iota(jnp.int32, (head_count, size), 0) // per_group
    position = lax.broadcasted_iota(jnp.int32, (head_count, positions), 1)

    def pick(values, index):
        result = values[0]
        for g in range(1, groups):
            result = jnp.where(index == g, values[g], result)
        return result

    for n in range(parts):
        large[n].wait()
        for s in range(n * part, (n + 1) * part):
            query = queries[s]
            scores = pick(
                [
                    lax.dot_general(
                        query, past[s, g, :, :size], (((1,), (1,)), ((), ())),
                        preferred_element_type=F32,
                    )
                    for g in range(groups)
                ],
                rows,
            ) * scaling
            keys = pick(
                [
                    jnp.broadcast_to(entry[s, g : g + 1, :size].astype(F32), (head_count, size))
                    for g in range(groups)
                ],
                owner,
            )
            own = jnp.sum(query.astype(F32) * keys, axis=1, keepdims=True) * scaling
            scores = jnp.where(position < lengths_ref[s], scores, -jnp.inf)
            highest = jnp.maximum(jnp.max(scores, axis=1, keepdims=True), own)
            weights = jnp.exp(scores - highest)
            own_weight = jnp.exp(own - highest)
            denominator = jnp.sum(weights, axis=1, keepdims=True) + own_weight
            low = (weights / denominator).astype(BF16)
            own_low = (own_weight / denominator).astype(BF16).astype(F32)
            mixed = pick(
                [
                    lax.dot_general(
                        low, past[s, g, :, size:], (((1,), (0,)), ((), ())),
                        preferred_element_type=F32,
                    )
                    for g in range(groups)
                ],
                owner,
            )
            values = pick(
                [
                    jnp.broadcast_to(entry[s, g : g + 1, size:].astype(F32), (head_count, size))
                    for g in range(groups)
                ],
                owner,
            )
            heads[s] = mixed + own_low * values
    for h in range(head_count):
        attn[:, h * size : (h + 1) * size] = heads[:, h, :].astype(BF16)
    store = pltpu.make_async_copy(attn, attn_hbm, sems.at[len(small) + parts])
    store.start()
    store.wait()


def front(
    queries, new_entry, past_entries, lengths, conv_state, mamba_input,
    conv_weight, conv_bias, state_proj, width,
):
    seqs, head_count, size = queries.shape
    channels = mamba_input.shape[1]
    outputs = state_proj.shape[0]
    spans = -(-outputs // width)
    vmem = lambda a: pltpu.VMEM(a.shape, a.dtype)
    bias = conv_bias.reshape(1, channels)
    return pl.pallas_call(
        functools.partial(front_kernel, width),
        out_shape=(
            jax.ShapeDtypeStruct((seqs, head_count * size), BF16),
            jax.ShapeDtypeStruct((seqs, channels), F32),
            jax.ShapeDtypeStruct((2 * spans * seqs, width), BF16),
        ),
        in_specs=[
            HBM_SPEC, HBM_SPEC, HBM_SPEC, pl.BlockSpec(memory_space=pltpu.SMEM),
            HBM_SPEC, HBM_SPEC, HBM_SPEC, HBM_SPEC, HBM_SPEC,
        ],
        out_specs=(HBM_SPEC, VMEM_SPEC, VMEM_SPEC),
        scratch_shapes=[
            vmem(past_entries), vmem(queries), vmem(new_entry), vmem(conv_state),
            vmem(mamba_input), vmem(conv_weight), vmem(bias), vmem(state_proj),
            pltpu.VMEM((seqs, head_count, size), F32),
            pltpu.VMEM((seqs, head_count * size), BF16),
            pltpu.SemaphoreType.DMA((16,)),
        ],
        cost_estimate=pl.CostEstimate(
            flops=6 * 10**9, bytes_accessed=4 * 10**6, transcendentals=0
        ),
        name="front",
    )(
        past_entries, queries, new_entry, lengths, conv_state, mamba_input,
        conv_weight, bias, state_proj,
    )


def expert_kernel(
    chunk, count, axes,
    gathered, *rest,
):
    peers, ways = axes
    tables = rest[:peers]
    inner_hbm, outer_hbm = rest[peers : peers + 2]
    outs = rest[peers + 2 : peers + 2 + ways]
    inner, outer, features, total, sems = rest[peers + 2 + ways :]
    experts, _, hidden_units, _ = inner.shape
    tokens = features.shape[0]
    width = gathered.shape[2]
    copies = []
    for e in range(experts):
        for c in range(count):
            span = pl.ds(c * chunk, chunk)
            group = []
            for n, (src, dst) in enumerate((
                (inner_hbm.at[e, 0, span], inner.at[e, 0, span]),
                (inner_hbm.at[e, 1, span], inner.at[e, 1, span]),
                (outer_hbm.at[e, span], outer.at[e, span]),
            )):
                group.append(pltpu.make_async_copy(src, dst, sems.at[e * count + c, n]))
            copies.append(group)
    for group in copies:
        for copy in group:
            copy.start()
    for t in range(ways):
        features[:, t * width : (t + 1) * width] = gathered[t, :tokens, :]
    table = jnp.concatenate([ref[:, width:].astype(F32) for ref in tables], axis=0)
    lane = lax.broadcasted_iota(jnp.int32, table.shape, 1)
    replicas = max(1, peers // EXPERTS)
    first = lax.axis_index("expert") * experts
    for e in range(experts):
        name = (first + e) // replicas
        chosen = (lane == name) | (lane == name + EXPERTS)
        gain = jnp.sum(jnp.where(chosen, table, 0.0), axis=1, keepdims=True)
        for c in range(count):
            group = copies[e * count + c]
            span = slice(c * chunk, (c + 1) * chunk)
            group[0].wait()
            gate = lax.dot_general(
                features[...], inner[e, 0, span], (((1,), (1,)), ((), ())),
                preferred_element_type=F32,
            )
            group[1].wait()
            up = lax.dot_general(
                features[...], inner[e, 1, span], (((1,), (1,)), ((), ())),
                preferred_element_type=F32,
            )
            hidden = (silu(gate) * up).astype(BF16)
            group[2].wait()
            value = gain * jnp.dot(hidden, outer[e, span], preferred_element_type=F32)
            if e == 0 and c == 0:
                total[...] = value
            else:
                total[...] += value
    me = lax.axis_index("tensor")
    for step in range(ways):
        start = pl.multiple_of(partner(me, step, ways) * width, LANES)
        outs[step][...] = total[:, pl.ds(start, width)].astype(outs[step].dtype)


def run_experts(gathered, packed, inner_weights, outer_weights):
    ways, rows, width = gathered.shape
    peers = len(packed)
    tokens = sum(p.shape[0] for p in packed)
    experts, _, hidden_units, features = inner_weights.shape
    chunk = min(512, hidden_units)
    count = hidden_units // chunk
    work = 6 * tokens * experts * hidden_units * features
    moved = 2 * (inner_weights.size + outer_weights.size)
    return pl.pallas_call(
        functools.partial(expert_kernel, chunk, count, (peers, ways)),
        out_shape=tuple(
            jax.ShapeDtypeStruct((tokens, width), F32 if step == 0 else BF16)
            for step in range(ways)
        ),
        in_specs=[VMEM_SPEC] * (1 + peers) + [HBM_SPEC, HBM_SPEC],
        out_specs=(VMEM_SPEC,) * ways,
        scratch_shapes=[
            pltpu.VMEM(inner_weights.shape, BF16),
            pltpu.VMEM(outer_weights.shape, BF16),
            pltpu.VMEM((tokens, features), BF16),
            pltpu.VMEM((tokens, features), F32),
            pltpu.SemaphoreType.DMA((experts * count, 3)),
        ],
        compiler_params=pltpu.CompilerParams(vmem_limit_bytes=56 * 2**20),
        cost_estimate=pl.CostEstimate(
            flops=work, bytes_accessed=moved, transcendentals=0
        ),
        name="experts",
    )(gathered, *packed, inner_weights, outer_weights)


def state_kernel(
    tokens, seqs, low_rank,
    gathered, act, gate, scan, step_proj, step_bias, decay, skip,
    out, next_state,
    square,
):
    ways, rows, width = gathered.shape
    states = decay.shape[0]
    spans = (rows - tokens) // (2 * seqs)
    pieces = []
    for span in range(spans):
        piece = None
        for t in range(ways):
            for half in range(2):
                row = tokens + (half * spans + span) * seqs
                part = gathered[t, row : row + seqs, :].astype(F32)
                piece = part if piece is None else piece + part
        pieces.append(piece)
    mixing = pieces[0] if spans == 1 else jnp.concatenate(pieces, axis=1)
    square[...] = jnp.zeros_like(square)
    square[:seqs, :] = mixing[:, low_rank : low_rank + LANES]
    columns = square[...].T
    step = (
        jnp.dot(mixing[:, :low_rank].astype(BF16), step_proj[...], preferred_element_type=F32)
        + step_bias[...]
    )
    step_size = jnp.maximum(step, 0.0) + jnp.log1p(jnp.exp(-jnp.abs(step)))
    rates = jnp.exp(decay[...])
    drive = step_size * act[...]
    results = []
    for s in range(seqs):
        in_coef = columns[:states, s : s + 1]
        out_coef = columns[states : 2 * states, s : s + 1]
        new = jnp.exp(-step_size[s : s + 1, :] * rates) * scan[s] + drive[s : s + 1, :] * in_coef
        next_state[s] = new
        results.append(jnp.sum(new * out_coef, axis=0, keepdims=True))
    mixed = jnp.concatenate(results, axis=0) + skip[...] * act[...]
    out[...] = (mixed * silu(gate[...].astype(F32))).astype(BF16)


def update_state(
    gathered, tokens, act, mamba_gate, scan_state, step_proj, step_bias, decay_log, skip_gain
):
    seqs, states, channels = scan_state.shape
    low_rank = step_proj.shape[0]
    block = min(512, channels)
    lane_block = lambda rows: pl.BlockSpec((rows, block), lambda c: (0, c))
    state_block = pl.BlockSpec((seqs, states, block), lambda c: (0, 0, c))
    return pl.pallas_call(
        functools.partial(state_kernel, tokens, seqs, low_rank),
        grid=(channels // block,),
        out_shape=(
            jax.ShapeDtypeStruct((seqs, channels), BF16),
            jax.ShapeDtypeStruct(scan_state.shape, F32),
        ),
        in_specs=[
            pl.BlockSpec(gathered.shape, lambda c: (0, 0, 0)),
            lane_block(seqs), lane_block(seqs), state_block,
            lane_block(low_rank), lane_block(1), lane_block(states), lane_block(1),
        ],
        out_specs=(lane_block(seqs), state_block),
        scratch_shapes=[pltpu.VMEM((LANES, LANES), F32)],
        cost_estimate=pl.CostEstimate(
            flops=3 * 10**9, bytes_accessed=3 * 10**6, transcendentals=0
        ),
        name="state",
    )(
        gathered, act, mamba_gate, scan_state, step_proj,
        step_bias.reshape(1, channels), decay_log, skip_gain.reshape(1, channels),
    )


def shards(
    mamba_input,
    mamba_gate,
    conv_state,
    scan_state,
    conv_weight,
    conv_bias,
    state_proj,
    step_proj,
    step_bias,
    decay_log,
    skip_gain,
    queries,
    new_entry,
    past_entries,
    lengths,
    expert_input,
    routes,
    slots,
    gates,
    inner_weights,
    outer_weights,
):
    del slots
    peers = lax.axis_size("expert")
    ways = lax.axis_size("tensor")
    seqs, width = expert_input.shape
    tokens = peers * seqs

    lane = lax.broadcasted_iota(jnp.int32, (seqs, LANES), 1)
    weight = jnp.zeros((seqs, LANES), F32)
    for k in range(routes.shape[1]):
        weight = weight + jnp.where(lane % EXPERTS == routes[:, k : k + 1], gates[:, k : k + 1], 0.0)
    high, low = split_bf16(weight)
    table = jnp.where(lane < EXPERTS, high, jnp.where(lane < 2 * EXPERTS, low, 0))
    packed = jnp.concatenate([expert_input, table.astype(BF16)], axis=1)
    packed = exchange([packed] * peers, "expert")

    attention_out, act, mix = front(
        queries, new_entry, past_entries, lengths, conv_state, mamba_input,
        conv_weight, conv_bias, state_proj, width,
    )
    mine = jnp.concatenate([p[:, :width] for p in packed] + [mix], axis=0)
    gathered = lax.all_gather(mine, "tensor", axis=0)
    partial = run_experts(gathered, packed, inner_weights, outer_weights)

    arrived = exchange(partial, "tensor")
    share = arrived[0]
    for part in arrived[1:]:
        share = share + part.astype(F32)
    mamba_out, next_state = update_state(
        gathered, tokens, act, mamba_gate, scan_state, step_proj, step_bias, decay_log, skip_gain
    )
    blocks = [share[n * seqs : (n + 1) * seqs] for n in range(peers)]
    blocks = [blocks[0]] + [block.astype(BF16) for block in blocks[1:]]
    returned = exchange(blocks, "expert", back=True)
    merged = returned[0]
    for part in returned[1:]:
        merged = merged + part.astype(F32)
    return (mamba_out, next_state, attention_out, merged.astype(BF16))


def solution(mesh):
    return jax.shard_map(
        shards,
        mesh=mesh,
        in_specs=(
            P(("parts", "expert"), "tensor"),
            P(("parts", "expert"), "tensor"),
            P(("parts", "expert"), None, "tensor"),
            P(("parts", "expert"), None, "tensor"),
            P(None, "tensor"),
            P("tensor"),
            P(None, "tensor"),
            P(None, "tensor"),
            P("tensor"),
            P(None, "tensor"),
            P("tensor"),
            P(("parts", "expert"), "tensor", None),
            P(("parts", "expert"), "tensor", None),
            P(("parts", "expert"), "tensor", None, None),
            P(("parts", "expert")),
            P(("parts", "expert"), "tensor"),
            P(("parts", "expert"), None),
            P(("parts", "expert"), None),
            P(("parts", "expert"), None),
            P("expert", None, "tensor", None),
            P("expert", "tensor", None),
        ),
        out_specs=(
            P(("parts", "expert"), "tensor"),
            P(("parts", "expert"), None, "tensor"),
            P(("parts", "expert"), "tensor"),
            P(("parts", "expert"), "tensor"),
        ),
        check_vma=False,
    )
```

```python
import functools

import jax
import jax.numpy as jnp
from jax import lax
from jax.experimental import pallas as pl
from jax.experimental.pallas import tpu as pltpu
from jax.sharding import PartitionSpec as P

EXPERTS = 8
LANES = 128
F32 = jnp.float32
BF16 = jnp.bfloat16

HBM_SPEC = pl.BlockSpec(memory_space=pl.ANY)
VMEM_SPEC = pl.BlockSpec(memory_space=pltpu.VMEM)


def silu(v):
    return v / (1.0 + jnp.exp(-v))


def split_bf16(v):
    high = v.astype(BF16)
    return high, (v - high.astype(F32)).astype(BF16)


def partner(index, step, count):
    if count & (count - 1) == 0:
        return index ^ step
    return (index + step) % count


def returner(index, step, count):
    if count & (count - 1) == 0:
        return index ^ step
    return (index - step) % count


def exchange(blocks, axis, back=False):
    count = lax.axis_size(axis)
    rule = returner if back else partner
    out = {0: blocks[0]}
    for step in range(count - 1, 0, -1):
        pairs = [(i, rule(i, step, count)) for i in range(count)]
        out[step] = lax.ppermute(blocks[step], axis, pairs)
    return [out[step] for step in range(count)]


def on_chip(value):
    return pltpu.with_memory_space_constraint(value, pltpu.VMEM)


def off_chip(*values):
    return [pltpu.with_memory_space_constraint(value, pltpu.HBM) for value in values]


def limit(mebibytes):
    return pltpu.CompilerParams(vmem_limit_bytes=mebibytes * 2**20)


def scratch_like(*arrays):
    return [pltpu.VMEM(a.shape, a.dtype) for a in arrays]


def pack_kernel(tokens_hbm, routes_hbm, gates_hbm, packed, tokens, routes, gates, square, sems):
    copies = [
        pltpu.make_async_copy(src, dst, sems.at[n])
        for n, (src, dst) in enumerate((
            (tokens_hbm, tokens), (routes_hbm, routes), (gates_hbm, gates)
        ))
    ]
    for copy in copies:
        copy.start()
    seqs, width = tokens.shape
    square[...] = jnp.zeros_like(square)
    row = lax.broadcasted_iota(jnp.int32, (LANES, seqs), 0)
    copies[1].wait()
    copies[2].wait()
    weight = jnp.zeros((LANES, seqs), F32)
    for k in range(routes.shape[0]):
        weight = weight + jnp.where(
            row % EXPERTS == routes[k : k + 1, :], gates[k : k + 1, :], 0.0
        )
    high = weight.astype(BF16).astype(F32)
    square[:, :seqs] = jnp.where(
        row < EXPERTS, high, jnp.where(row < 2 * EXPERTS, weight - high, 0.0)
    )
    packed[:, width:] = square[...].T[:seqs, :].astype(BF16)
    copies[0].wait()
    packed[:, :width] = tokens[...]


def pack(expert_input, routes, gates):
    seqs, width = expert_input.shape
    operands = (expert_input, routes.T, gates.T)
    return pl.pallas_call(
        pack_kernel,
        out_shape=pltpu.VMEM((seqs, width + LANES), BF16),
        in_specs=[HBM_SPEC] * 3,
        out_specs=VMEM_SPEC,
        scratch_shapes=scratch_like(*operands) + [
            pltpu.VMEM((LANES, LANES), F32), pltpu.SemaphoreType.DMA((3,)),
        ],
        compiler_params=limit(4),
        name="pack",
    )(*off_chip(*operands))


def front_kernel(
    width, ready, chunk,
    state_hbm, input_hbm, taps_hbm, bias_hbm, proj_hbm, inner_hbm, outer_hbm,
    act_ref, mix_ref, inner, outer,
    state, inputs, taps, bias, proj, sems,
):
    small = [
        pltpu.make_async_copy(src, dst, sems.at[n])
        for n, (src, dst) in enumerate((
            (state_hbm, state), (input_hbm, inputs), (taps_hbm, taps),
            (bias_hbm, bias), (proj_hbm, proj),
        ))
    ]
    large = []
    for c in range(ready):
        span = pl.ds(c * chunk, chunk)
        for n, (src, dst) in enumerate((
            (inner_hbm.at[0, 0, span], inner.at[c, 0]),
            (inner_hbm.at[0, 1, span], inner.at[c, 1]),
            (outer_hbm.at[0, span], outer.at[c]),
        )):
            large.append(
                pltpu.make_async_copy(src, dst, sems.at[len(small) + 3 * c + n])
            )
    for copy in small + large:
        copy.start()
    for copy in small[:4]:
        copy.wait()
    seqs = inputs.shape[0]
    total = bias[...]
    for k in range(taps.shape[0] - 1):
        total = total + state[k].astype(F32) * taps[k : k + 1, :]
    total = total + inputs[...].astype(F32) * taps[taps.shape[0] - 1 :, :]
    act = silu(total)
    act_ref[...] = act
    small[4].wait()
    mix = lax.dot_general(
        act.astype(BF16), proj[...], (((1,), (1,)), ((), ())), preferred_element_type=F32
    )
    outputs = mix.shape[1]
    spans = -(-outputs // width)
    row = 0
    for piece in split_bf16(mix):
        for span in range(spans):
            cut = piece[:, span * width : min(outputs, (span + 1) * width)]
            if cut.shape[1] < width:
                cut = jnp.concatenate(
                    [cut.astype(F32), jnp.zeros((seqs, width - cut.shape[1]), F32)], axis=1
                ).astype(BF16)
            mix_ref[row : row + seqs, :] = cut
            row += seqs
    for copy in large:
        copy.wait()


def front(
    conv_state, mamba_input, conv_weight, conv_bias, state_proj, inner_weights, outer_weights,
    width, ready, chunk,
):
    seqs, channels = mamba_input.shape
    features = inner_weights.shape[3]
    spans = -(-state_proj.shape[0] // width)
    operands = (
        jnp.swapaxes(conv_state, 0, 1), mamba_input, conv_weight,
        conv_bias.reshape(1, channels), state_proj,
    )
    return pl.pallas_call(
        functools.partial(front_kernel, width, ready, chunk),
        out_shape=(
            pltpu.VMEM((seqs, channels), F32),
            pltpu.VMEM((2 * spans * seqs, width), BF16),
            pltpu.VMEM((ready, 2, chunk, features), BF16),
            pltpu.VMEM((ready, chunk, features), BF16),
        ),
        in_specs=[HBM_SPEC] * 7,
        out_specs=(VMEM_SPEC,) * 4,
        scratch_shapes=scratch_like(*operands) + [
            pltpu.SemaphoreType.DMA((len(operands) + 3 * ready,)),
        ],
        compiler_params=limit(4),
        cost_estimate=pl.CostEstimate(
            flops=4 * 10**9, bytes_accessed=14 * 10**6, transcendentals=0
        ),
        name="front",
    )(*off_chip(*operands, inner_weights, outer_weights))


def attend_kernel(
    past_hbm, queries_hbm, entry_hbm, lengths_ref, out_hbm,
    past, queries, entry, scores, own, heads, out, sems,
):
    seqs, head_count, size = queries.shape
    groups = entry.shape[1]
    per_group = head_count // groups
    positions = past.shape[1] // groups
    parts = 4 if seqs % 4 == 0 else 1
    part = seqs // parts
    small = [
        pltpu.make_async_copy(queries_hbm, queries, sems.at[parts]),
        pltpu.make_async_copy(entry_hbm, entry, sems.at[parts + 1]),
    ]
    large = [
        pltpu.make_async_copy(
            past_hbm.at[pl.ds(n * part, part)], past.at[pl.ds(n * part, part)], sems.at[n]
        )
        for n in range(parts)
    ]
    for copy in small + large:
        copy.start()
    scaling = size ** (-0.5)
    group_of = lambda lanes: lax.broadcasted_iota(jnp.int32, (head_count, lanes), 0) // per_group
    position = lax.broadcasted_iota(jnp.int32, (head_count, positions), 1)

    def pick(values, index):
        result = values[0]
        for g in range(1, groups):
            result = jnp.where(index == g, values[g], result)
        return result

    def entry_rows(s, lanes):
        return pick(
            [
                jnp.broadcast_to(entry[s, g : g + 1, lanes].astype(F32), (head_count, size))
                for g in range(groups)
            ],
            group_of(size),
        )

    for copy in small:
        copy.wait()
    for n in range(parts):
        large[n].wait()
        for s in range(n * part, (n + 1) * part):
            every = lax.dot_general(
                queries[s], past[s, :, :size], (((1,), (1,)), ((), ())),
                preferred_element_type=F32,
            )
            mine = pick(
                [every[:, g * positions : (g + 1) * positions] for g in range(groups)],
                group_of(positions),
            )
            scores[s] = jnp.where(position < lengths_ref[s], mine * scaling, -jnp.inf)
            own[s] = queries[s].astype(F32) * entry_rows(s, slice(0, size))
    score = scores[...]
    own_score = jnp.sum(own[...], axis=2, keepdims=True) * scaling
    highest = jnp.maximum(jnp.max(score, axis=2, keepdims=True), own_score)
    weights = jnp.exp(score - highest)
    own_weight = jnp.exp(own_score - highest)
    denominator = jnp.sum(weights, axis=2, keepdims=True) + own_weight
    scores[...] = weights / denominator
    own[...] = jnp.broadcast_to(own_weight / denominator, own.shape)
    for s in range(seqs):
        low = scores[s]
        spread = [
            jnp.where(group_of(positions) == g, low, 0.0).astype(BF16) for g in range(groups)
        ]
        spread = spread[0] if groups == 1 else jnp.concatenate(spread, axis=1)
        mixed = jnp.dot(spread, past[s, :, size:], preferred_element_type=F32)
        heads[s] = mixed + own[s].astype(BF16).astype(F32) * entry_rows(s, slice(size, None))
    for h in range(head_count):
        out[:, h * size : (h + 1) * size] = heads[:, h, :].astype(BF16)
    store = pltpu.make_async_copy(out, out_hbm, sems.at[parts + 2])
    store.start()
    store.wait()


def attend(queries, new_entry, past_entries, lengths):
    seqs, head_count, size = queries.shape
    past = past_entries.reshape(seqs, -1, 2 * size)
    positions = past_entries.shape[2]
    return pl.pallas_call(
        attend_kernel,
        out_shape=jax.ShapeDtypeStruct((seqs, head_count * size), BF16),
        in_specs=[HBM_SPEC, HBM_SPEC, HBM_SPEC, pl.BlockSpec(memory_space=pltpu.SMEM)],
        out_specs=HBM_SPEC,
        scratch_shapes=scratch_like(past, queries, new_entry) + [
            pltpu.VMEM((seqs, head_count, positions), F32),
            pltpu.VMEM((seqs, head_count, size), F32),
            pltpu.VMEM((seqs, head_count, size), F32),
            pltpu.VMEM((seqs, head_count * size), BF16),
            pltpu.SemaphoreType.DMA((8,)),
        ],
        compiler_params=limit(8),
        cost_estimate=pl.CostEstimate(
            flops=4 * 10**9, bytes_accessed=2 * 10**6, transcendentals=0
        ),
        name="attend",
    )(*off_chip(past, queries, new_entry), lengths)


def expert_kernel(chunk, ready, peers, ways, gathered, *rest):
    tables = rest[:peers]
    inner_ready, outer_ready, inner_hbm, outer_hbm = rest[peers : peers + 4]
    outs = rest[peers + 4 : peers + 4 + ways]
    inner, outer, features, hidden, total, sems = rest[peers + 4 + ways :]
    experts, _, hidden_units, _ = inner_hbm.shape
    count = hidden_units // chunk
    tokens = features.shape[0]
    width = gathered.shape[2]
    copies = []
    for step in range(ready, experts * count):
        e, c = divmod(step, count)
        span = pl.ds(c * chunk, chunk)
        slot = step - ready
        copies.append([
            pltpu.make_async_copy(src, dst, sems.at[slot, n])
            for n, (src, dst) in enumerate((
                (inner_hbm.at[e, 0, span], inner.at[slot, 0]),
                (inner_hbm.at[e, 1, span], inner.at[slot, 1]),
                (outer_hbm.at[e, span], outer.at[slot]),
            ))
        ])
    for group in copies:
        for copy in group:
            copy.start()
    for t in range(ways):
        features[:, t * width : (t + 1) * width] = gathered[t, :tokens, :]
    table = jnp.concatenate([ref[:, width:].astype(F32) for ref in tables], axis=0)
    lane = lax.broadcasted_iota(jnp.int32, table.shape, 1)
    replicas = max(1, peers // EXPERTS)
    first = lax.axis_index("expert") * experts
    piece = min(256, chunk)
    contract = (((1,), (1,)), ((), ()))
    for step in range(experts * count):
        e, c = divmod(step, count)
        if c == 0:
            name = (first + e) // replicas
            chosen = (lane == name) | (lane == name + EXPERTS)
            gain = jnp.sum(jnp.where(chosen, table, 0.0), axis=1, keepdims=True)
        if step < ready:
            weights, down = inner_ready.at[step], outer_ready.at[step]
        else:
            weights, down = inner.at[step - ready], outer.at[step - ready]
            for copy in copies[step - ready]:
                copy.wait()
        for p in range(0, chunk, piece):
            gate = lax.dot_general(
                weights[0, p : p + piece], features[...], contract, preferred_element_type=F32
            )
            up = lax.dot_general(
                weights[1, p : p + piece], features[...], contract, preferred_element_type=F32
            )
            hidden[p : p + piece, :] = (silu(gate) * up).astype(BF16)
        value = gain * lax.dot_general(
            hidden[...], down[...], (((0,), (0,)), ((), ())), preferred_element_type=F32
        )
        if step == 0:
            total[...] = value
        else:
            total[...] += value
    me = lax.axis_index("tensor")
    for step in range(ways):
        start = pl.multiple_of(partner(me, step, ways) * width, LANES)
        outs[step][...] = total[:, pl.ds(start, width)].astype(outs[step].dtype)


def run_experts(gathered, packed, inner_ready, outer_ready, inner_weights, outer_weights):
    ways, rows, width = gathered.shape
    peers = len(packed)
    tokens = sum(p.shape[0] for p in packed)
    experts, _, hidden_units, features = inner_weights.shape
    ready, chunk, _ = outer_ready.shape
    left = max(1, experts * hidden_units // chunk - ready)
    work = 6 * tokens * experts * hidden_units * features
    moved = 2 * (inner_weights.size + outer_weights.size)
    return pl.pallas_call(
        functools.partial(expert_kernel, chunk, ready, peers, ways),
        out_shape=tuple(
            pltpu.VMEM((tokens, width), F32 if step == 0 else BF16) for step in range(ways)
        ),
        in_specs=[VMEM_SPEC] * (3 + peers) + [HBM_SPEC, HBM_SPEC],
        out_specs=(VMEM_SPEC,) * ways,
        scratch_shapes=[
            pltpu.VMEM((left, 2, chunk, features), BF16),
            pltpu.VMEM((left, chunk, features), BF16),
            pltpu.VMEM((tokens, features), BF16),
            pltpu.VMEM((chunk, tokens), BF16),
            pltpu.VMEM((tokens, features), F32),
            pltpu.SemaphoreType.DMA((left, 3)),
        ],
        compiler_params=limit(44),
        cost_estimate=pl.CostEstimate(
            flops=work, bytes_accessed=moved, transcendentals=0
        ),
        name="experts",
    )(
        on_chip(gathered), *[on_chip(p) for p in packed], on_chip(inner_ready),
        on_chip(outer_ready), *off_chip(inner_weights, outer_weights),
    )


def state_kernel(
    tokens, seqs, low_rank,
    gathered, act, gate, scan, step_proj, step_bias, decay, skip,
    out, next_state,
    square,
):
    ways, rows, width = gathered.shape
    states = decay.shape[0]
    spans = (rows - tokens) // (2 * seqs)
    pieces = []
    for span in range(spans):
        piece = None
        for t in range(ways):
            for half in range(2):
                row = tokens + (half * spans + span) * seqs
                part = gathered[t, row : row + seqs, :].astype(F32)
                piece = part if piece is None else piece + part
        pieces.append(piece)
    mixing = pieces[0] if spans == 1 else jnp.concatenate(pieces, axis=1)
    square[...] = jnp.zeros_like(square)
    square[:seqs, :] = mixing[:, low_rank : low_rank + LANES]
    columns = square[...].T
    step = (
        jnp.dot(mixing[:, :low_rank].astype(BF16), step_proj[...], preferred_element_type=F32)
        + step_bias[...]
    )
    step_size = jnp.maximum(step, 0.0) + jnp.log1p(jnp.exp(-jnp.abs(step)))
    rates = jnp.exp(decay[...])
    drive = step_size * act[...]
    results = []
    for s in range(seqs):
        in_coef = columns[:states, s : s + 1]
        out_coef = columns[states : 2 * states, s : s + 1]
        new = jnp.exp(-step_size[s : s + 1, :] * rates) * scan[s] + drive[s : s + 1, :] * in_coef
        next_state[s] = new
        results.append(jnp.sum(new * out_coef, axis=0, keepdims=True))
    mixed = jnp.concatenate(results, axis=0) + skip[...] * act[...]
    out[...] = (mixed * silu(gate[...].astype(F32))).astype(BF16)


def update_state(
    gathered, tokens, act, mamba_gate, scan_state, step_proj, step_bias, decay_log, skip_gain
):
    seqs, states, channels = scan_state.shape
    low_rank = step_proj.shape[0]
    block = min(512, channels)
    lane_block = lambda rows: pl.BlockSpec((rows, block), lambda c: (0, c))
    state_block = pl.BlockSpec((seqs, states, block), lambda c: (0, 0, c))
    return pl.pallas_call(
        functools.partial(state_kernel, tokens, seqs, low_rank),
        grid=(channels // block,),
        out_shape=(
            jax.ShapeDtypeStruct((seqs, channels), BF16),
            jax.ShapeDtypeStruct(scan_state.shape, F32),
        ),
        in_specs=[
            pl.BlockSpec(gathered.shape, lambda c: (0, 0, 0)),
            lane_block(seqs), lane_block(seqs), state_block,
            lane_block(low_rank), lane_block(1), lane_block(states), lane_block(1),
        ],
        out_specs=(lane_block(seqs), state_block),
        scratch_shapes=[pltpu.VMEM((LANES, LANES), F32)],
        compiler_params=limit(12),
        cost_estimate=pl.CostEstimate(
            flops=3 * 10**9, bytes_accessed=3 * 10**6, transcendentals=0
        ),
        name="state",
    )(
        gathered, act, mamba_gate, scan_state, step_proj,
        step_bias.reshape(1, channels), decay_log, skip_gain.reshape(1, channels),
    )


def shards(
    mamba_input,
    mamba_gate,
    conv_state,
    scan_state,
    conv_weight,
    conv_bias,
    state_proj,
    step_proj,
    step_bias,
    decay_log,
    skip_gain,
    queries,
    new_entry,
    past_entries,
    lengths,
    expert_input,
    routes,
    slots,
    gates,
    inner_weights,
    outer_weights,
):
    del slots
    peers = lax.axis_size("expert")
    ways = lax.axis_size("tensor")
    seqs, width = expert_input.shape
    tokens = peers * seqs

    hidden_units = inner_weights.shape[2]
    chunk = min(512, hidden_units)
    ready = min(2, hidden_units // chunk)

    packed = exchange([pack(expert_input, routes, gates)] * peers, "expert")
    act, mix, inner_ready, outer_ready = front(
        conv_state, mamba_input, conv_weight, conv_bias, state_proj,
        inner_weights, outer_weights, width, ready, chunk,
    )
    mine = jnp.concatenate([p[:, :width] for p in packed] + [mix], axis=0)
    gathered = lax.all_gather(mine, "tensor", axis=0)
    partial = run_experts(
        gathered, packed, inner_ready, outer_ready, inner_weights, outer_weights
    )

    arrived = exchange(partial, "tensor")
    attention_out = attend(queries, new_entry, past_entries, lengths)
    share = arrived[0]
    for part in arrived[1:]:
        share = share + part.astype(F32)
    mamba_out, next_state = update_state(
        gathered, tokens, act, mamba_gate, scan_state, step_proj, step_bias, decay_log, skip_gain
    )
    blocks = [share[n * seqs : (n + 1) * seqs] for n in range(peers)]
    blocks = [blocks[0]] + [block.astype(BF16) for block in blocks[1:]]
    returned = exchange(blocks, "expert", back=True)
    merged = returned[0]
    for part in returned[1:]:
        merged = merged + part.astype(F32)
    return (mamba_out, next_state, attention_out, merged.astype(BF16))


def solution(mesh):
    return jax.shard_map(
        shards,
        mesh=mesh,
        in_specs=(
            P(("parts", "expert"), "tensor"),
            P(("parts", "expert"), "tensor"),
            P(("parts", "expert"), None, "tensor"),
            P(("parts", "expert"), None, "tensor"),
            P(None, "tensor"),
            P("tensor"),
            P(None, "tensor"),
            P(None, "tensor"),
            P("tensor"),
            P(None, "tensor"),
            P("tensor"),
            P(("parts", "expert"), "tensor", None),
            P(("parts", "expert"), "tensor", None),
            P(("parts", "expert"), "tensor", None, None),
            P(("parts", "expert")),
            P(("parts", "expert"), "tensor"),
            P(("parts", "expert"), None),
            P(("parts", "expert"), None),
            P(("parts", "expert"), None),
            P("expert", None, "tensor", None),
            P("expert", "tensor", None),
        ),
        out_specs=(
            P(("parts", "expert"), "tensor"),
            P(("parts", "expert"), None, "tensor"),
            P(("parts", "expert"), "tensor"),
            P(("parts", "expert"), "tensor"),
        ),
        check_vma=False,
    )
```

```python
import functools

import jax
import jax.numpy as jnp
from jax import lax
from jax.experimental import pallas as pl
from jax.experimental.pallas import tpu as pltpu
from jax.sharding import PartitionSpec as P

EXPERTS = 8
LANES = 128
F32 = jnp.float32
BF16 = jnp.bfloat16

HBM_SPEC = pl.BlockSpec(memory_space=pl.ANY)
VMEM_SPEC = pl.BlockSpec(memory_space=pltpu.VMEM)


def silu(v):
    return v / (1.0 + jnp.exp(-v))


def split_bf16(v):
    high = v.astype(BF16)
    return high, (v - high.astype(F32)).astype(BF16)


def partner(index, step, count):
    if count & (count - 1) == 0:
        return index ^ step
    return (index + step) % count


def returner(index, step, count):
    if count & (count - 1) == 0:
        return index ^ step
    return (index - step) % count


def exchange(blocks, axis, back=False):
    count = lax.axis_size(axis)
    rule = returner if back else partner
    out = {0: blocks[0]}
    for step in range(count - 1, 0, -1):
        pairs = [(i, rule(i, step, count)) for i in range(count)]
        out[step] = lax.ppermute(blocks[step], axis, pairs)
    return [out[step] for step in range(count)]


def on_chip(value):
    return pltpu.with_memory_space_constraint(value, pltpu.VMEM)


def off_chip(*values):
    return [pltpu.with_memory_space_constraint(value, pltpu.HBM) for value in values]


def limit(mebibytes):
    return pltpu.CompilerParams(vmem_limit_bytes=mebibytes * 2**20)


def scratch_like(*arrays):
    return [pltpu.VMEM(a.shape, a.dtype) for a in arrays]


def pack_kernel(tokens_hbm, routes_hbm, gates_hbm, packed, tokens, routes, gates, square, sems):
    copies = [
        pltpu.make_async_copy(src, dst, sems.at[n])
        for n, (src, dst) in enumerate((
            (tokens_hbm, tokens), (routes_hbm, routes), (gates_hbm, gates)
        ))
    ]
    for copy in copies:
        copy.start()
    seqs, width = tokens.shape
    square[...] = jnp.zeros_like(square)
    row = lax.broadcasted_iota(jnp.int32, (LANES, seqs), 0)
    copies[1].wait()
    copies[2].wait()
    weight = jnp.zeros((LANES, seqs), F32)
    for k in range(routes.shape[0]):
        weight = weight + jnp.where(
            row % EXPERTS == routes[k : k + 1, :], gates[k : k + 1, :], 0.0
        )
    high = weight.astype(BF16).astype(F32)
    square[:, :seqs] = jnp.where(
        row < EXPERTS, high, jnp.where(row < 2 * EXPERTS, weight - high, 0.0)
    )
    packed[:, width:] = square[...].T[:seqs, :].astype(BF16)
    copies[0].wait()
    packed[:, :width] = tokens[...]


def pack(expert_input, routes, gates):
    seqs, width = expert_input.shape
    operands = (expert_input, routes.T, gates.T)
    return pl.pallas_call(
        pack_kernel,
        out_shape=pltpu.VMEM((seqs, width + LANES), BF16),
        in_specs=[HBM_SPEC] * 3,
        out_specs=VMEM_SPEC,
        scratch_shapes=scratch_like(*operands) + [
            pltpu.VMEM((LANES, LANES), F32), pltpu.SemaphoreType.DMA((3,)),
        ],
        compiler_params=limit(1),
        cost_estimate=pl.CostEstimate(
            flops=60*10**9, bytes_accessed=10**5, transcendentals=0
        ),
        name="pack",
    )(*off_chip(*operands))


def front_kernel(
    width,
    state_hbm, input_hbm, taps_hbm, bias_hbm, proj_hbm,
    act_ref, mix_ref,
    state, inputs, taps, bias, proj, sems,
):
    copies = [
        pltpu.make_async_copy(src, dst, sems.at[n])
        for n, (src, dst) in enumerate((
            (state_hbm, state), (input_hbm, inputs), (taps_hbm, taps),
            (bias_hbm, bias), (proj_hbm, proj),
        ))
    ]
    for copy in copies:
        copy.start()
    for copy in copies[:4]:
        copy.wait()
    seqs = inputs.shape[0]
    total = bias[...]
    for k in range(taps.shape[0] - 1):
        total = total + state[k].astype(F32) * taps[k : k + 1, :]
    total = total + inputs[...].astype(F32) * taps[taps.shape[0] - 1 :, :]
    act = silu(total)
    act_ref[...] = act
    copies[4].wait()
    mix = lax.dot_general(
        act.astype(BF16), proj[...], (((1,), (1,)), ((), ())), preferred_element_type=F32
    )
    outputs = mix.shape[1]
    spans = -(-outputs // width)
    row = 0
    for piece in split_bf16(mix):
        for span in range(spans):
            cut = piece[:, span * width : min(outputs, (span + 1) * width)]
            if cut.shape[1] < width:
                cut = jnp.concatenate(
                    [cut.astype(F32), jnp.zeros((seqs, width - cut.shape[1]), F32)], axis=1
                ).astype(BF16)
            mix_ref[row : row + seqs, :] = cut
            row += seqs


def front(conv_state, mamba_input, conv_weight, conv_bias, state_proj, width):
    seqs, channels = mamba_input.shape
    spans = -(-state_proj.shape[0] // width)
    operands = (
        jnp.swapaxes(conv_state, 0, 1), mamba_input, conv_weight,
        conv_bias.reshape(1, channels), state_proj,
    )
    return pl.pallas_call(
        functools.partial(front_kernel, width),
        out_shape=(
            pltpu.VMEM((seqs, channels), F32),
            pltpu.VMEM((2 * spans * seqs, width), BF16),
        ),
        in_specs=[HBM_SPEC] * len(operands),
        out_specs=(VMEM_SPEC,) * 2,
        scratch_shapes=scratch_like(*operands) + [
            pltpu.SemaphoreType.DMA((len(operands),)),
        ],
        compiler_params=limit(4),
        cost_estimate=pl.CostEstimate(
            flops=1*10**9, bytes_accessed=10**6, transcendentals=0
        ),
        name="front",
    )(*off_chip(*operands))


def join_kernel(*refs):
    *blocks, mix, out = refs
    row = 0
    for block in blocks:
        rows = block.shape[0]
        out[row : row + rows, :] = block[:, : out.shape[1]]
        row += rows
    out[row:, :] = mix[...]


def join(packed, mix):
    rows = sum(p.shape[0] for p in packed) + mix.shape[0]
    return pl.pallas_call(
        join_kernel,
        out_shape=pltpu.VMEM((rows, mix.shape[1]), BF16),
        in_specs=[VMEM_SPEC] * (len(packed) + 1),
        out_specs=VMEM_SPEC,
        compiler_params=limit(1),
        name="join",
    )(*[on_chip(p) for p in packed], on_chip(mix))


def attend_kernel(
    past_hbm, queries_hbm, entry_hbm, lengths_ref, out_hbm,
    past, queries, entry, scores, own, heads, out, sems,
):
    seqs, head_count, size = queries.shape
    groups = entry.shape[1]
    per_group = head_count // groups
    positions = past.shape[1] // groups
    parts = 4 if seqs % 4 == 0 else 1
    part = seqs // parts
    small = [
        pltpu.make_async_copy(queries_hbm, queries, sems.at[parts]),
        pltpu.make_async_copy(entry_hbm, entry, sems.at[parts + 1]),
    ]
    large = [
        pltpu.make_async_copy(
            past_hbm.at[pl.ds(n * part, part)], past.at[pl.ds(n * part, part)], sems.at[n]
        )
        for n in range(parts)
    ]
    for copy in small + large:
        copy.start()
    scaling = size ** (-0.5)
    group_of = lambda lanes: lax.broadcasted_iota(jnp.int32, (head_count, lanes), 0) // per_group
    position = lax.broadcasted_iota(jnp.int32, (head_count, positions), 1)

    def pick(values, index):
        result = values[0]
        for g in range(1, groups):
            result = jnp.where(index == g, values[g], result)
        return result

    def entry_rows(s, lanes):
        return pick(
            [
                jnp.broadcast_to(entry[s, g : g + 1, lanes].astype(F32), (head_count, size))
                for g in range(groups)
            ],
            group_of(size),
        )

    for copy in small:
        copy.wait()
    for n in range(parts):
        large[n].wait()
        for s in range(n * part, (n + 1) * part):
            every = lax.dot_general(
                queries[s], past[s, :, :size], (((1,), (1,)), ((), ())),
                preferred_element_type=F32,
            )
            mine = pick(
                [every[:, g * positions : (g + 1) * positions] for g in range(groups)],
                group_of(positions),
            )
            scores[s] = jnp.where(position < lengths_ref[s], mine * scaling, -jnp.inf)
            own[s] = queries[s].astype(F32) * entry_rows(s, slice(0, size))
    score = scores[...]
    own_score = jnp.sum(own[...], axis=2, keepdims=True) * scaling
    highest = jnp.maximum(jnp.max(score, axis=2, keepdims=True), own_score)
    weights = jnp.exp(score - highest)
    own_weight = jnp.exp(own_score - highest)
    denominator = jnp.sum(weights, axis=2, keepdims=True) + own_weight
    scores[...] = weights / denominator
    own[...] = jnp.broadcast_to(own_weight / denominator, own.shape)
    for s in range(seqs):
        low = scores[s]
        spread = [
            jnp.where(group_of(positions) == g, low, 0.0).astype(BF16) for g in range(groups)
        ]
        spread = spread[0] if groups == 1 else jnp.concatenate(spread, axis=1)
        mixed = jnp.dot(spread, past[s, :, size:], preferred_element_type=F32)
        heads[s] = mixed + own[s].astype(BF16).astype(F32) * entry_rows(s, slice(size, None))
    for h in range(head_count):
        out[:, h * size : (h + 1) * size] = heads[:, h, :].astype(BF16)
    store = pltpu.make_async_copy(out, out_hbm, sems.at[parts + 2])
    store.start()
    store.wait()


def attend(queries, new_entry, past_entries, lengths):
    seqs, head_count, size = queries.shape
    past = past_entries.reshape(seqs, -1, 2 * size)
    positions = past_entries.shape[2]
    return pl.pallas_call(
        attend_kernel,
        out_shape=jax.ShapeDtypeStruct((seqs, head_count * size), BF16),
        in_specs=[HBM_SPEC, HBM_SPEC, HBM_SPEC, pl.BlockSpec(memory_space=pltpu.SMEM)],
        out_specs=HBM_SPEC,
        scratch_shapes=scratch_like(past, queries, new_entry) + [
            pltpu.VMEM((seqs, head_count, positions), F32),
            pltpu.VMEM((seqs, head_count, size), F32),
            pltpu.VMEM((seqs, head_count, size), F32),
            pltpu.VMEM((seqs, head_count * size), BF16),
            pltpu.SemaphoreType.DMA((8,)),
        ],
        compiler_params=limit(8),
        cost_estimate=pl.CostEstimate(
            flops=4 * 10**9, bytes_accessed=2 * 10**6, transcendentals=0
        ),
        name="attend",
    )(*off_chip(past, queries, new_entry), lengths)


def expert_kernel(chunk, peers, ways, gathered, *rest):
    tables = rest[:peers]
    inner, outer = rest[peers : peers + 2]
    outs = rest[peers + 2 : peers + 2 + ways]
    features, total = rest[peers + 2 + ways :]
    experts, _, hidden_units, _ = inner.shape
    count = hidden_units // chunk
    steps = [(e, slice(c * chunk, (c + 1) * chunk)) for e in range(experts) for c in range(count)]
    tokens = features.shape[0]
    width = gathered.shape[2]
    for t in range(ways):
        features[:, t * width : (t + 1) * width] = gathered[t, :tokens, :]
    table = jnp.concatenate([ref[:, width:].astype(F32) for ref in tables], axis=0)
    lane = lax.broadcasted_iota(jnp.int32, table.shape, 1)
    replicas = max(1, peers // EXPERTS)
    first = lax.axis_index("expert") * experts
    gains = []
    for e in range(experts):
        name = (first + e) // replicas
        chosen = (lane == name) | (lane == name + EXPERTS)
        gains.append(jnp.sum(jnp.where(chosen, table, 0.0), axis=1, keepdims=True))
    contract = (((1,), (1,)), ((), ()))

    def hidden(step):
        e, span = steps[step]
        gate = lax.dot_general(
            inner[e, 0, span], features[...], contract, preferred_element_type=F32
        )
        up = lax.dot_general(
            inner[e, 1, span], features[...], contract, preferred_element_type=F32
        )
        return (silu(gate) * up).astype(BF16)

    ahead = hidden(0)
    for step in range(len(steps)):
        e, span = steps[step]
        now = ahead
        if step + 1 < len(steps):
            ahead = hidden(step + 1)
        value = gains[e] * lax.dot_general(
            now, outer[e, span], (((0,), (0,)), ((), ())), preferred_element_type=F32
        )
        if step == 0:
            total[...] = value
        else:
            total[...] += value
    me = lax.axis_index("tensor")
    for step in range(ways):
        start = pl.multiple_of(partner(me, step, ways) * width, LANES)
        outs[step][...] = total[:, pl.ds(start, width)].astype(outs[step].dtype)


def run_experts(gathered, packed, inner_weights, outer_weights):
    ways, rows, width = gathered.shape
    peers = len(packed)
    tokens = sum(p.shape[0] for p in packed)
    experts, _, hidden_units, features = inner_weights.shape
    chunk = min(512, hidden_units)
    work = 6 * tokens * experts * hidden_units * features
    moved = 2 * (inner_weights.size + outer_weights.size)
    return pl.pallas_call(
        functools.partial(expert_kernel, chunk, peers, ways),
        out_shape=tuple(
            pltpu.VMEM((tokens, width), F32 if step == 0 else BF16) for step in range(ways)
        ),
        in_specs=[VMEM_SPEC] * (3 + peers),
        out_specs=(VMEM_SPEC,) * ways,
        scratch_shapes=[
            pltpu.VMEM((tokens, features), BF16),
            pltpu.VMEM((tokens, features), F32),
        ],
        compiler_params=limit(8),
        cost_estimate=pl.CostEstimate(
            flops=work, bytes_accessed=moved, transcendentals=0
        ),
        name="experts",
    )(
        on_chip(gathered), *[on_chip(p) for p in packed], on_chip(inner_weights),
        on_chip(outer_weights),
    )


def state_kernel(
    tokens, seqs, low_rank,
    gathered, act, gate, scan, step_proj, step_bias, decay, skip,
    out, next_state,
    square,
):
    ways, rows, width = gathered.shape
    states = decay.shape[0]
    spans = (rows - tokens) // (2 * seqs)
    pieces = []
    for span in range(spans):
        piece = None
        for t in range(ways):
            for half in range(2):
                row = tokens + (half * spans + span) * seqs
                part = gathered[t, row : row + seqs, :].astype(F32)
                piece = part if piece is None else piece + part
        pieces.append(piece)
    mixing = pieces[0] if spans == 1 else jnp.concatenate(pieces, axis=1)
    square[...] = jnp.zeros_like(square)
    square[:seqs, :] = mixing[:, low_rank : low_rank + LANES]
    columns = square[...].T
    step = (
        jnp.dot(mixing[:, :low_rank].astype(BF16), step_proj[...], preferred_element_type=F32)
        + step_bias[...]
    )
    step_size = jnp.maximum(step, 0.0) + jnp.log1p(jnp.exp(-jnp.abs(step)))
    rates = jnp.exp(decay[...])
    drive = step_size * act[...]
    results = []
    for s in range(seqs):
        in_coef = columns[:states, s : s + 1]
        out_coef = columns[states : 2 * states, s : s + 1]
        new = jnp.exp(-step_size[s : s + 1, :] * rates) * scan[s] + drive[s : s + 1, :] * in_coef
        next_state[s] = new
        results.append(jnp.sum(new * out_coef, axis=0, keepdims=True))
    mixed = jnp.concatenate(results, axis=0) + skip[...] * act[...]
    out[...] = (mixed * silu(gate[...].astype(F32))).astype(BF16)


def update_state(
    gathered, tokens, act, mamba_gate, scan_state, step_proj, step_bias, decay_log, skip_gain
):
    seqs, states, channels = scan_state.shape
    low_rank = step_proj.shape[0]
    block = min(512, channels)
    lane_block = lambda rows: pl.BlockSpec((rows, block), lambda c: (0, c))
    state_block = pl.BlockSpec((seqs, states, block), lambda c: (0, 0, c))
    return pl.pallas_call(
        functools.partial(state_kernel, tokens, seqs, low_rank),
        grid=(channels // block,),
        out_shape=(
            jax.ShapeDtypeStruct((seqs, channels), BF16),
            jax.ShapeDtypeStruct(scan_state.shape, F32),
        ),
        in_specs=[
            pl.BlockSpec(gathered.shape, lambda c: (0, 0, 0)),
            lane_block(seqs), lane_block(seqs), state_block,
            lane_block(low_rank), lane_block(1), lane_block(states), lane_block(1),
        ],
        out_specs=(lane_block(seqs), state_block),
        scratch_shapes=[pltpu.VMEM((LANES, LANES), F32)],
        compiler_params=limit(12),
        cost_estimate=pl.CostEstimate(
            flops=3 * 10**9, bytes_accessed=3 * 10**6, transcendentals=0
        ),
        name="state",
    )(
        gathered, act, mamba_gate, scan_state, step_proj,
        step_bias.reshape(1, channels), decay_log, skip_gain.reshape(1, channels),
    )


def shards(
    mamba_input,
    mamba_gate,
    conv_state,
    scan_state,
    conv_weight,
    conv_bias,
    state_proj,
    step_proj,
    step_bias,
    decay_log,
    skip_gain,
    queries,
    new_entry,
    past_entries,
    lengths,
    expert_input,
    routes,
    slots,
    gates,
    inner_weights,
    outer_weights,
):
    del slots
    peers = lax.axis_size("expert")
    ways = lax.axis_size("tensor")
    seqs, width = expert_input.shape
    tokens = peers * seqs

    packed = exchange([pack(expert_input, routes, gates)] * peers, "expert")
    act, mix = front(conv_state, mamba_input, conv_weight, conv_bias, state_proj, width)
    mine = join(packed, mix)
    gathered = lax.all_gather(mine, "tensor", axis=0)
    partial = run_experts(gathered, packed, inner_weights, outer_weights)

    arrived = exchange(partial, "tensor")
    attention_out = attend(queries, new_entry, past_entries, lengths)
    share = arrived[0]
    for part in arrived[1:]:
        share = share + part.astype(F32)
    mamba_out, next_state = update_state(
        gathered, tokens, act, mamba_gate, scan_state, step_proj, step_bias, decay_log, skip_gain
    )
    blocks = [share[n * seqs : (n + 1) * seqs] for n in range(peers)]
    blocks = [blocks[0]] + [block.astype(BF16) for block in blocks[1:]]
    returned = exchange(blocks, "expert", back=True)
    merged = returned[0]
    for part in returned[1:]:
        merged = merged + part.astype(F32)
    return (mamba_out, next_state, attention_out, merged.astype(BF16))


def solution(mesh):
    return jax.shard_map(
        shards,
        mesh=mesh,
        in_specs=(
            P(("parts", "expert"), "tensor"),
            P(("parts", "expert"), "tensor"),
            P(("parts", "expert"), None, "tensor"),
            P(("parts", "expert"), None, "tensor"),
            P(None, "tensor"),
            P("tensor"),
            P(None, "tensor"),
            P(None, "tensor"),
            P("tensor"),
            P(None, "tensor"),
            P("tensor"),
            P(("parts", "expert"), "tensor", None),
            P(("parts", "expert"), "tensor", None),
            P(("parts", "expert"), "tensor", None, None),
            P(("parts", "expert")),
            P(("parts", "expert"), "tensor"),
            P(("parts", "expert"), None),
            P(("parts", "expert"), None),
            P(("parts", "expert"), None),
            P("expert", None, "tensor", None),
            P("expert", "tensor", None),
        ),
        out_specs=(
            P(("parts", "expert"), "tensor"),
            P(("parts", "expert"), None, "tensor"),
            P(("parts", "expert"), "tensor"),
            P(("parts", "expert"), "tensor"),
        ),
        check_vma=False,
    )
```

```python
import functools

import jax
import jax.numpy as jnp
from jax import lax
from jax.experimental import pallas as pl
from jax.experimental.pallas import tpu as pltpu
from jax.sharding import PartitionSpec as P


EXPERTS = 8
LANES = 128
F32 = jnp.float32
BF16 = jnp.bfloat16

HBM_SPEC = pl.BlockSpec(memory_space=pl.ANY)
VMEM_SPEC = pl.BlockSpec(memory_space=pltpu.VMEM)


def silu(v):
    return v / (1.0 + jnp.exp(-v))


def partner(index, step, count):
    if count & (count - 1) == 0:
        return index ^ step
    return (index + step) % count


def returner(index, step, count):
    if count & (count - 1) == 0:
        return index ^ step
    return (index - step) % count


def exchange(blocks, axis, back=False):
    count = lax.axis_size(axis)
    rule = returner if back else partner
    out = {0: blocks[0]}
    for step in range(count - 1, 0, -1):
        pairs = [(i, rule(i, step, count)) for i in range(count)]
        out[step] = lax.ppermute(blocks[step], axis, pairs)
    return [out[step] for step in range(count)]


def on_chip(value):
    return pltpu.with_memory_space_constraint(value, pltpu.VMEM)


def off_chip(*values):
    return [pltpu.with_memory_space_constraint(value, pltpu.HBM) for value in values]


def limit(mebibytes):
    return pltpu.CompilerParams(vmem_limit_bytes=mebibytes * 2**20)


def scratch_like(*arrays):
    return [pltpu.VMEM(a.shape, a.dtype) for a in arrays]


def pack_kernel(tokens_hbm, routes_hbm, gates_hbm, packed, tokens, routes, gates, square, sems):
    copies = [
        pltpu.make_async_copy(src, dst, sems.at[n])
        for n, (src, dst) in enumerate((
            (tokens_hbm, tokens), (routes_hbm, routes), (gates_hbm, gates)
        ))
    ]
    for copy in copies:
        copy.start()
    seqs, width = tokens.shape
    square[...] = jnp.zeros_like(square)
    row = lax.broadcasted_iota(jnp.int32, (LANES, seqs), 0)
    copies[1].wait()
    copies[2].wait()
    weight = jnp.zeros((LANES, seqs), F32)
    for k in range(routes.shape[0]):
        weight = weight + jnp.where(
            row % EXPERTS == routes[k : k + 1, :], gates[k : k + 1, :], 0.0
        )
    high = weight.astype(BF16).astype(F32)
    square[:, :seqs] = jnp.where(
        row < EXPERTS, high, jnp.where(row < 2 * EXPERTS, weight - high, 0.0)
    )
    packed[:, width:] = square[...].T[:seqs, :].astype(BF16)
    copies[0].wait()
    packed[:, :width] = tokens[...]


def pack(expert_input, routes, gates):
    seqs, width = expert_input.shape
    operands = (expert_input, routes.T, gates.T)
    return pl.pallas_call(
        pack_kernel,
        out_shape=pltpu.VMEM((seqs, width + LANES), BF16),
        in_specs=[HBM_SPEC] * 3,
        out_specs=VMEM_SPEC,
        scratch_shapes=scratch_like(*operands) + [
            pltpu.VMEM((LANES, LANES), F32), pltpu.SemaphoreType.DMA((3,)),
        ],
        compiler_params=limit(1),
        cost_estimate=pl.CostEstimate(
            flops=60*10**9, bytes_accessed=10**5, transcendentals=0
        ),
        name="pack",
    )(*off_chip(*operands))


def front_kernel(
    width,
    state_hbm, input_hbm, taps_hbm, bias_hbm, proj_hbm,
    act_ref, mix_ref,
    state, inputs, taps, bias, proj, sems,
):
    copies = [
        pltpu.make_async_copy(src, dst, sems.at[n])
        for n, (src, dst) in enumerate((
            (state_hbm, state), (input_hbm, inputs), (taps_hbm, taps),
            (bias_hbm, bias), (proj_hbm, proj),
        ))
    ]
    for copy in copies:
        copy.start()
    for copy in copies[:4]:
        copy.wait()
    seqs = inputs.shape[0]
    total = bias[...]
    for k in range(taps.shape[0] - 1):
        total = total + state[k].astype(F32) * taps[k : k + 1, :]
    total = total + inputs[...].astype(F32) * taps[taps.shape[0] - 1 :, :]
    act = silu(total)
    act_ref[...] = act
    copies[4].wait()
    mix = lax.dot_general(
        act.astype(BF16), proj[...], (((1,), (1,)), ((), ())), preferred_element_type=F32
    )
    outputs = mix.shape[1]
    spans = -(-outputs // width)
    row = 0
    for piece in (mix.astype(BF16),):
        for span in range(spans):
            cut = piece[:, span * width : min(outputs, (span + 1) * width)]
            if cut.shape[1] < width:
                cut = jnp.concatenate(
                    [cut.astype(F32), jnp.zeros((seqs, width - cut.shape[1]), F32)], axis=1
                ).astype(BF16)
            mix_ref[row : row + seqs, :] = cut
            row += seqs


def front(conv_state, mamba_input, conv_weight, conv_bias, state_proj, width):
    seqs, channels = mamba_input.shape
    spans = -(-state_proj.shape[0] // width)
    operands = (
        jnp.swapaxes(conv_state, 0, 1), mamba_input, conv_weight,
        conv_bias.reshape(1, channels), state_proj,
    )
    return pl.pallas_call(
        functools.partial(front_kernel, width),
        out_shape=(
            pltpu.VMEM((seqs, channels), F32),
            pltpu.VMEM((spans * seqs, width), BF16),
        ),
        in_specs=[HBM_SPEC] * len(operands),
        out_specs=(VMEM_SPEC,) * 2,
        scratch_shapes=scratch_like(*operands) + [
            pltpu.SemaphoreType.DMA((len(operands),)),
        ],
        compiler_params=limit(4),
        cost_estimate=pl.CostEstimate(
            flops=1*10**9, bytes_accessed=10**6, transcendentals=0
        ),
        name="front",
    )(*off_chip(*operands))


def join_kernel(*refs):
    *blocks, mix, out = refs
    row = 0
    for block in blocks:
        rows = block.shape[0]
        out[row : row + rows, :] = block[:, : out.shape[1]]
        row += rows
    out[row:, :] = mix[...]


def join(packed, mix):
    rows = sum(p.shape[0] for p in packed) + mix.shape[0]
    return pl.pallas_call(
        join_kernel,
        out_shape=pltpu.VMEM((rows, mix.shape[1]), BF16),
        in_specs=[VMEM_SPEC] * (len(packed) + 1),
        out_specs=VMEM_SPEC,
        compiler_params=limit(1),
        name="join",
    )(*[on_chip(p) for p in packed], on_chip(mix))


def attend_kernel(
    past, queries, entry, lengths_ref, out_hbm,
    scores, own, heads, out, sem,
):
    seqs, head_count, size = queries.shape
    groups = entry.shape[1]
    per_group = head_count // groups
    positions = past.shape[1] // groups
    scaling = size ** (-0.5)
    group_of = lambda lanes: lax.broadcasted_iota(jnp.int32, (head_count, lanes), 0) // per_group
    position = lax.broadcasted_iota(jnp.int32, (head_count, positions), 1)

    def pick(values, index):
        result = values[0]
        for g in range(1, groups):
            result = jnp.where(index == g, values[g], result)
        return result

    def entry_rows(s, lanes):
        return pick(
            [
                jnp.broadcast_to(entry[s, g : g + 1, lanes].astype(F32), (head_count, size))
                for g in range(groups)
            ],
            group_of(size),
        )

    for s in range(seqs):
        every = lax.dot_general(
            queries[s], past[s, :, :size], (((1,), (1,)), ((), ())),
            preferred_element_type=F32,
        )
        mine = pick(
            [every[:, g * positions : (g + 1) * positions] for g in range(groups)],
            group_of(positions),
        )
        scores[s] = jnp.where(position < lengths_ref[s], mine * scaling, -jnp.inf)
        own[s] = queries[s].astype(F32) * entry_rows(s, slice(0, size))
    score = scores[...]
    own_score = jnp.sum(own[...], axis=2, keepdims=True) * scaling
    highest = jnp.maximum(jnp.max(score, axis=2, keepdims=True), own_score)
    weights = jnp.exp(score - highest)
    own_weight = jnp.exp(own_score - highest)
    denominator = jnp.sum(weights, axis=2, keepdims=True) + own_weight
    scores[...] = weights / denominator
    own[...] = jnp.broadcast_to(own_weight / denominator, own.shape)
    for s in range(seqs):
        low = scores[s]
        spread = [
            jnp.where(group_of(positions) == g, low, 0.0).astype(BF16) for g in range(groups)
        ]
        spread = spread[0] if groups == 1 else jnp.concatenate(spread, axis=1)
        mixed = jnp.dot(spread, past[s, :, size:], preferred_element_type=F32)
        heads[s] = mixed + own[s].astype(BF16).astype(F32) * entry_rows(s, slice(size, None))
    for h in range(head_count):
        out[:, h * size : (h + 1) * size] = heads[:, h, :].astype(BF16)
    store = pltpu.make_async_copy(out, out_hbm, sem)
    store.start()
    store.wait()


def attend(queries, new_entry, past_entries, lengths):
    seqs, head_count, size = queries.shape
    past = past_entries.reshape(seqs, -1, 2 * size)
    positions = past_entries.shape[2]
    return pl.pallas_call(
        attend_kernel,
        out_shape=jax.ShapeDtypeStruct((seqs, head_count * size), BF16),
        in_specs=[VMEM_SPEC] * 3 + [pl.BlockSpec(memory_space=pltpu.SMEM)],
        out_specs=HBM_SPEC,
        scratch_shapes=[
            pltpu.VMEM((seqs, head_count, positions), F32),
            pltpu.VMEM((seqs, head_count, size), F32),
            pltpu.VMEM((seqs, head_count, size), F32),
            pltpu.VMEM((seqs, head_count * size), BF16),
            pltpu.SemaphoreType.DMA,
        ],
        compiler_params=limit(4),
        cost_estimate=pl.CostEstimate(
            flops=4 * 10**9, bytes_accessed=2 * 10**6, transcendentals=0
        ),
        name="attend",
    )(on_chip(past), on_chip(queries), on_chip(new_entry), lengths)


def weight_columns(tables, width, experts, peers):
    table = jnp.concatenate([ref[:, width:].astype(F32) for ref in tables], axis=0)
    lane = lax.broadcasted_iota(jnp.int32, table.shape, 1)
    replicas = max(1, peers // EXPERTS)
    first = lax.axis_index("expert") * experts
    columns = []
    for e in range(experts):
        name = (first + e) // replicas
        chosen = (lane == name) | (lane == name + EXPERTS)
        columns.append(jnp.sum(jnp.where(chosen, table, 0.0), axis=1, keepdims=True))
    return columns


def project_down(hidden, outer, gains, outs, steps, ways, width):
    me = lax.axis_index("tensor")
    for out, step in zip(outs, steps):
        start = pl.multiple_of(partner(me, step, ways) * width, LANES)
        total = None
        for e, gain in enumerate(gains):
            value = gain * lax.dot_general(
                hidden[e], outer[e, :, pl.ds(start, width)], (((0,), (0,)), ((), ())),
                preferred_element_type=F32,
            )
            total = value if total is None else total + value
        out[...] = total.astype(out.dtype)


def hidden_kernel(chunk, gathered, inner, hidden, features):
    experts, _, hidden_units, _ = inner.shape
    ways, _, width = gathered.shape
    tokens = features.shape[0]
    for t in range(ways):
        features[:, t * width : (t + 1) * width] = gathered[t, :tokens, :]
    contract = (((1,), (1,)), ((), ()))
    for e in range(experts):
        for c in range(0, hidden_units, chunk):
            span = slice(c, c + chunk)
            gate = lax.dot_general(
                inner[e, 0, span], features[...], contract, preferred_element_type=F32
            )
            up = lax.dot_general(
                inner[e, 1, span], features[...], contract, preferred_element_type=F32
            )
            hidden[e, span] = (silu(gate) * up).astype(BF16)


def down_kernel(peers, ways, steps, hidden, outer, *rest):
    tables, outs = rest[:peers], rest[peers:]
    width = outs[0].shape[1]
    gains = weight_columns(tables, width, outer.shape[0], peers)
    project_down(hidden, outer, gains, outs, steps, ways, width)


def run_experts(gathered, packed, inner_weights, outer_weights):
    ways, _, width = gathered.shape
    peers = len(packed)
    tokens = sum(p.shape[0] for p in packed)
    experts, _, hidden_units, features = inner_weights.shape
    chunk = min(512, hidden_units)
    work = 2 * tokens * experts * hidden_units * features
    hidden = pl.pallas_call(
        functools.partial(hidden_kernel, chunk),
        out_shape=pltpu.VMEM((experts, hidden_units, tokens), BF16),
        in_specs=[VMEM_SPEC] * 2,
        out_specs=VMEM_SPEC,
        scratch_shapes=[pltpu.VMEM((tokens, features), BF16)],
        compiler_params=limit(6),
        cost_estimate=pl.CostEstimate(
            flops=10**8, bytes_accessed=10**5, transcendentals=0
        ),
        name="hidden",
    )(on_chip(gathered), on_chip(inner_weights))
    operands = (on_chip(hidden), on_chip(outer_weights), *[on_chip(p) for p in packed])

    def down(steps):
        return pl.pallas_call(
            functools.partial(down_kernel, peers, ways, steps),
            out_shape=tuple(
                pltpu.VMEM((tokens, width), F32 if step == 0 else BF16) for step in steps
            ),
            in_specs=[VMEM_SPEC] * len(operands),
            out_specs=(VMEM_SPEC,) * len(steps),
            compiler_params=limit(6),
            cost_estimate=pl.CostEstimate(
                flops=work // 2, bytes_accessed=outer_weights.size, transcendentals=0
            ),
        )(*operands)

    half = max(1, ways // 2)
    far = down(list(range(half, ways)))
    near = down(list(range(half)))
    return [*near, *far]


def state_kernel(
    tokens, seqs, low_rank,
    gathered, act, gate, scan, step_proj, step_bias, decay, skip,
    out, next_state,
    square,
):
    ways, rows, _ = gathered.shape
    states = decay.shape[0]
    spans = (rows - tokens) // seqs
    pieces = []
    for span in range(spans):
        piece = None
        for t in range(ways):
            row = tokens + span * seqs
            part = gathered[t, row : row + seqs, :].astype(F32)
            piece = part if piece is None else piece + part
        pieces.append(piece)
    mixing = pieces[0] if spans == 1 else jnp.concatenate(pieces, axis=1)
    square[...] = jnp.zeros_like(square)
    square[:seqs, :] = mixing[:, low_rank : low_rank + LANES]
    columns = square[...].T
    step = (
        jnp.dot(mixing[:, :low_rank].astype(BF16), step_proj[...], preferred_element_type=F32)
        + step_bias[...]
    )
    step_size = jnp.maximum(step, 0.0) + jnp.log1p(jnp.exp(-jnp.abs(step)))
    rates = jnp.exp(decay[...])
    drive = step_size * act[...]
    results = []
    for s in range(seqs):
        in_coef = columns[:states, s : s + 1]
        out_coef = columns[states : 2 * states, s : s + 1]
        new = jnp.exp(-step_size[s : s + 1, :] * rates) * scan[s] + drive[s : s + 1, :] * in_coef
        next_state[s] = new
        results.append(jnp.sum(new * out_coef, axis=0, keepdims=True))
    mixed = jnp.concatenate(results, axis=0) + skip[...] * act[...]
    out[...] = (mixed * silu(gate[...].astype(F32))).astype(BF16)


def update_state(
    gathered, tokens, act, mamba_gate, scan_state, step_proj, step_bias, decay_log, skip_gain
):
    seqs, states, channels = scan_state.shape
    low_rank = step_proj.shape[0]
    block = min(512, channels)
    lane_block = lambda rows: pl.BlockSpec((rows, block), lambda c: (0, c))
    state_block = pl.BlockSpec((seqs, states, block), lambda c: (0, 0, c))
    return pl.pallas_call(
        functools.partial(state_kernel, tokens, seqs, low_rank),
        grid=(channels // block,),
        out_shape=(
            jax.ShapeDtypeStruct((seqs, channels), BF16),
            jax.ShapeDtypeStruct(scan_state.shape, F32),
        ),
        in_specs=[
            pl.BlockSpec(gathered.shape, lambda c: (0, 0, 0)),
            lane_block(seqs), lane_block(seqs), state_block,
            lane_block(low_rank), lane_block(1), lane_block(states), lane_block(1),
        ],
        out_specs=(lane_block(seqs), state_block),
        scratch_shapes=[pltpu.VMEM((LANES, LANES), F32)],
        compiler_params=limit(12),
        cost_estimate=pl.CostEstimate(
            flops=3 * 10**9, bytes_accessed=3 * 10**6, transcendentals=0
        ),
        name="state",
    )(
        gathered, act, mamba_gate, scan_state, step_proj,
        step_bias.reshape(1, channels), decay_log, skip_gain.reshape(1, channels),
    )


def shards(
    mamba_input,
    mamba_gate,
    conv_state,
    scan_state,
    conv_weight,
    conv_bias,
    state_proj,
    step_proj,
    step_bias,
    decay_log,
    skip_gain,
    queries,
    new_entry,
    past_entries,
    lengths,
    expert_input,
    routes,
    slots,
    gates,
    inner_weights,
    outer_weights,
):
    del slots
    peers = lax.axis_size("expert")
    seqs, width = expert_input.shape
    tokens = peers * seqs

    packed = exchange([pack(expert_input, routes, gates)] * peers, "expert")
    act, mix = front(conv_state, mamba_input, conv_weight, conv_bias, state_proj, width)
    mine = join(packed, mix)
    gathered = lax.all_gather(mine, "tensor", axis=0)
    partial = run_experts(gathered, packed, inner_weights, outer_weights)

    arrived = exchange(partial, "tensor")
    attention_out = attend(queries, new_entry, past_entries, lengths)
    share = arrived[0]
    for part in arrived[1:]:
        share = share + part.astype(F32)
    mamba_out, next_state = update_state(
        gathered, tokens, act, mamba_gate, scan_state, step_proj, step_bias, decay_log, skip_gain
    )
    blocks = [share[n * seqs : (n + 1) * seqs] for n in range(peers)]
    blocks = [blocks[0]] + [block.astype(BF16) for block in blocks[1:]]
    returned = exchange(blocks, "expert", back=True)
    merged = returned[0]
    for part in returned[1:]:
        merged = merged + part.astype(F32)
    return (mamba_out, next_state, attention_out, merged.astype(BF16))


def solution(mesh):
    return jax.shard_map(
        shards,
        mesh=mesh,
        in_specs=(
            P(("parts", "expert"), "tensor"),
            P(("parts", "expert"), "tensor"),
            P(("parts", "expert"), None, "tensor"),
            P(("parts", "expert"), None, "tensor"),
            P(None, "tensor"),
            P("tensor"),
            P(None, "tensor"),
            P(None, "tensor"),
            P("tensor"),
            P(None, "tensor"),
            P("tensor"),
            P(("parts", "expert"), "tensor", None),
            P(("parts", "expert"), "tensor", None),
            P(("parts", "expert"), "tensor", None, None),
            P(("parts", "expert")),
            P(("parts", "expert"), "tensor"),
            P(("parts", "expert"), None),
            P(("parts", "expert"), None),
            P(("parts", "expert"), None),
            P("expert", None, "tensor", None),
            P("expert", "tensor", None),
        ),
        out_specs=(
            P(("parts", "expert"), "tensor"),
            P(("parts", "expert"), None, "tensor"),
            P(("parts", "expert"), "tensor"),
            P(("parts", "expert"), "tensor"),
        ),
        check_vma=False,
    )
```

```python
import functools

import jax
import jax.numpy as jnp
from jax import lax
from jax.experimental import pallas as pl
from jax.experimental.pallas import tpu as pltpu
from jax.sharding import PartitionSpec as P


EXPERTS = 8
LANES = 128
F32 = jnp.float32
BF16 = jnp.bfloat16

HBM_SPEC = pl.BlockSpec(memory_space=pl.ANY)
VMEM_SPEC = pl.BlockSpec(memory_space=pltpu.VMEM)


def silu(v):
    return v / (1.0 + jnp.exp(-v))


def partner(index, step, count):
    if count & (count - 1) == 0:
        return index ^ step
    return (index + step) % count


def returner(index, step, count):
    if count & (count - 1) == 0:
        return index ^ step
    return (index - step) % count


def exchange(blocks, axis, back=False):
    count = lax.axis_size(axis)
    rule = returner if back else partner
    out = {0: blocks[0]}
    for step in range(count - 1, 0, -1):
        pairs = [(i, rule(i, step, count)) for i in range(count)]
        out[step] = lax.ppermute(blocks[step], axis, pairs)
    return [out[step] for step in range(count)]


def on_chip(value):
    return pltpu.with_memory_space_constraint(value, pltpu.VMEM)


def off_chip(*values):
    return [pltpu.with_memory_space_constraint(value, pltpu.HBM) for value in values]


def limit(mebibytes):
    return pltpu.CompilerParams(vmem_limit_bytes=mebibytes * 2**20)


def scratch_like(*arrays):
    return [pltpu.VMEM(a.shape, a.dtype) for a in arrays]


def pack_kernel(tokens_hbm, routes_hbm, gates_hbm, packed, tokens, routes, gates, square, sems):
    copies = [
        pltpu.make_async_copy(src, dst, sems.at[n])
        for n, (src, dst) in enumerate((
            (tokens_hbm, tokens), (routes_hbm, routes), (gates_hbm, gates)
        ))
    ]
    for copy in copies:
        copy.start()
    seqs, width = tokens.shape
    square[...] = jnp.zeros_like(square)
    row = lax.broadcasted_iota(jnp.int32, (LANES, seqs), 0)
    copies[1].wait()
    copies[2].wait()
    weight = jnp.zeros((LANES, seqs), F32)
    for k in range(routes.shape[0]):
        weight = weight + jnp.where(
            row % EXPERTS == routes[k : k + 1, :], gates[k : k + 1, :], 0.0
        )
    high = weight.astype(BF16).astype(F32)
    square[:, :seqs] = jnp.where(
        row < EXPERTS, high, jnp.where(row < 2 * EXPERTS, weight - high, 0.0)
    )
    packed[:, width:] = square[...].T[:seqs, :].astype(BF16)
    copies[0].wait()
    packed[:, :width] = tokens[...]


def pack(expert_input, routes, gates):
    seqs, width = expert_input.shape
    operands = (expert_input, routes.T, gates.T)
    return pl.pallas_call(
        pack_kernel,
        out_shape=pltpu.VMEM((seqs, width + LANES), BF16),
        in_specs=[HBM_SPEC] * 3,
        out_specs=VMEM_SPEC,
        scratch_shapes=scratch_like(*operands) + [
            pltpu.VMEM((LANES, LANES), F32), pltpu.SemaphoreType.DMA((3,)),
        ],
        compiler_params=limit(1),
        cost_estimate=pl.CostEstimate(
            flops=60*10**9, bytes_accessed=10**5, transcendentals=0
        ),
        name="pack",
    )(*off_chip(*operands))


def front_kernel(
    width,
    state_hbm, input_hbm, taps_hbm, bias_hbm, proj_hbm,
    act_ref, mix_ref,
    state, inputs, taps, bias, proj, sems,
):
    copies = [
        pltpu.make_async_copy(src, dst, sems.at[n])
        for n, (src, dst) in enumerate((
            (state_hbm, state), (input_hbm, inputs), (taps_hbm, taps),
            (bias_hbm, bias), (proj_hbm, proj),
        ))
    ]
    for copy in copies:
        copy.start()
    for copy in copies[:4]:
        copy.wait()
    seqs = inputs.shape[0]
    total = bias[...]
    for k in range(taps.shape[0] - 1):
        total = total + state[k].astype(F32) * taps[k : k + 1, :]
    total = total + inputs[...].astype(F32) * taps[taps.shape[0] - 1 :, :]
    act = silu(total)
    act_ref[...] = act
    copies[4].wait()
    mix = lax.dot_general(
        act.astype(BF16), proj[...], (((1,), (1,)), ((), ())), preferred_element_type=F32
    )
    outputs = mix.shape[1]
    spans = -(-outputs // width)
    row = 0
    for piece in (mix.astype(BF16),):
        for span in range(spans):
            cut = piece[:, span * width : min(outputs, (span + 1) * width)]
            if cut.shape[1] < width:
                cut = jnp.concatenate(
                    [cut.astype(F32), jnp.zeros((seqs, width - cut.shape[1]), F32)], axis=1
                ).astype(BF16)
            mix_ref[row : row + seqs, :] = cut
            row += seqs


def front(conv_state, mamba_input, conv_weight, conv_bias, state_proj, width):
    seqs, channels = mamba_input.shape
    spans = -(-state_proj.shape[0] // width)
    operands = (
        jnp.swapaxes(conv_state, 0, 1), mamba_input, conv_weight,
        conv_bias.reshape(1, channels), state_proj,
    )
    return pl.pallas_call(
        functools.partial(front_kernel, width),
        out_shape=(
            pltpu.VMEM((seqs, channels), F32),
            pltpu.VMEM((spans * seqs, width), BF16),
        ),
        in_specs=[HBM_SPEC] * len(operands),
        out_specs=(VMEM_SPEC,) * 2,
        scratch_shapes=scratch_like(*operands) + [
            pltpu.SemaphoreType.DMA((len(operands),)),
        ],
        compiler_params=limit(4),
        cost_estimate=pl.CostEstimate(
            flops=10*10**9, bytes_accessed=10**6, transcendentals=0
        ),
        name="front",
    )(*off_chip(*operands))


def join_kernel(*refs):
    *blocks, mix, out = refs
    row = 0
    for block in blocks:
        rows = block.shape[0]
        out[row : row + rows, :] = block[:, : out.shape[1]]
        row += rows
    out[row:, :] = mix[...]


def join(packed, mix):
    rows = sum(p.shape[0] for p in packed) + mix.shape[0]
    return pl.pallas_call(
        join_kernel,
        out_shape=pltpu.VMEM((rows, mix.shape[1]), BF16),
        in_specs=[VMEM_SPEC] * (len(packed) + 1),
        out_specs=VMEM_SPEC,
        compiler_params=limit(1),
        name="join",
    )(*[on_chip(p) for p in packed], on_chip(mix))


def attend_kernel(
    past, queries, entry, lengths_ref, out,
    scores, own, heads,
):
    seqs, head_count, size = queries.shape
    groups = entry.shape[1]
    per_group = head_count // groups
    positions = past.shape[1] // groups
    scaling = size ** (-0.5)
    group_of = lambda lanes: lax.broadcasted_iota(jnp.int32, (head_count, lanes), 0) // per_group
    position = lax.broadcasted_iota(jnp.int32, (head_count, positions), 1)

    def pick(values, index):
        result = values[0]
        for g in range(1, groups):
            result = jnp.where(index == g, values[g], result)
        return result

    def entry_rows(s, lanes):
        return pick(
            [
                jnp.broadcast_to(entry[s, g : g + 1, lanes].astype(F32), (head_count, size))
                for g in range(groups)
            ],
            group_of(size),
        )

    for s in range(seqs):
        every = lax.dot_general(
            queries[s], past[s, :, :size], (((1,), (1,)), ((), ())),
            preferred_element_type=F32,
        )
        mine = pick(
            [every[:, g * positions : (g + 1) * positions] for g in range(groups)],
            group_of(positions),
        )
        scores[s] = jnp.where(position < lengths_ref[s], mine * scaling, -jnp.inf)
        own[s] = queries[s].astype(F32) * entry_rows(s, slice(0, size))
    score = scores[...]
    own_score = jnp.sum(own[...], axis=2, keepdims=True) * scaling
    highest = jnp.maximum(jnp.max(score, axis=2, keepdims=True), own_score)
    weights = jnp.exp(score - highest)
    own_weight = jnp.exp(own_score - highest)
    denominator = jnp.sum(weights, axis=2, keepdims=True) + own_weight
    scores[...] = weights / denominator
    own[...] = jnp.broadcast_to(own_weight / denominator, own.shape)
    for s in range(seqs):
        low = scores[s]
        spread = [
            jnp.where(group_of(positions) == g, low, 0.0).astype(BF16) for g in range(groups)
        ]
        spread = spread[0] if groups == 1 else jnp.concatenate(spread, axis=1)
        mixed = jnp.dot(spread, past[s, :, size:], preferred_element_type=F32)
        heads[s] = mixed + own[s].astype(BF16).astype(F32) * entry_rows(s, slice(size, None))
    for h in range(head_count):
        out[:, h * size : (h + 1) * size] = heads[:, h, :].astype(BF16)


def attend(queries, new_entry, past_entries, lengths):
    seqs, head_count, size = queries.shape
    past = past_entries.reshape(seqs, -1, 2 * size)
    positions = past_entries.shape[2]
    return pl.pallas_call(
        attend_kernel,
        out_shape=pltpu.VMEM((seqs, head_count * size), BF16),
        in_specs=[VMEM_SPEC] * 3 + [pl.BlockSpec(memory_space=pltpu.SMEM)],
        out_specs=VMEM_SPEC,
        scratch_shapes=[
            pltpu.VMEM((seqs, head_count, positions), F32),
            pltpu.VMEM((seqs, head_count, size), F32),
            pltpu.VMEM((seqs, head_count, size), F32),
        ],
        compiler_params=limit(4),
        cost_estimate=pl.CostEstimate(
            flops=4 * 10**9, bytes_accessed=2 * 10**6, transcendentals=0
        ),
        name="attend",
    )(on_chip(past), on_chip(queries), on_chip(new_entry), lengths)


def weight_columns(tables, width, experts, peers):
    table = jnp.concatenate([ref[:, width:].astype(F32) for ref in tables], axis=0)
    lane = lax.broadcasted_iota(jnp.int32, table.shape, 1)
    replicas = max(1, peers // EXPERTS)
    first = lax.axis_index("expert") * experts
    columns = []
    for e in range(experts):
        name = (first + e) // replicas
        chosen = (lane == name) | (lane == name + EXPERTS)
        columns.append(jnp.sum(jnp.where(chosen, table, 0.0), axis=1, keepdims=True))
    return columns


def project_down(hidden, outer, gains, outs, steps, ways, width):
    me = lax.axis_index("tensor")
    for out, step in zip(outs, steps):
        start = pl.multiple_of(partner(me, step, ways) * width, LANES)
        total = None
        for e, gain in enumerate(gains):
            value = gain * lax.dot_general(
                hidden[e], outer[e, :, pl.ds(start, width)], (((0,), (0,)), ((), ())),
                preferred_element_type=F32,
            )
            total = value if total is None else total + value
        out[...] = total.astype(out.dtype)


def hidden_kernel(chunk, gathered, inner, hidden, features):
    experts, _, hidden_units, _ = inner.shape
    ways, _, width = gathered.shape
    tokens = features.shape[0]
    for t in range(ways):
        features[:, t * width : (t + 1) * width] = gathered[t, :tokens, :]
    contract = (((1,), (1,)), ((), ()))
    for e in range(experts):
        for c in range(0, hidden_units, chunk):
            span = slice(c, c + chunk)
            gate = lax.dot_general(
                inner[e, 0, span], features[...], contract, preferred_element_type=F32
            )
            up = lax.dot_general(
                inner[e, 1, span], features[...], contract, preferred_element_type=F32
            )
            hidden[e, span] = (silu(gate) * up).astype(BF16)


def down_kernel(peers, ways, steps, hidden, outer, *rest):
    tables, outs = rest[:peers], rest[peers:]
    width = outs[0].shape[1]
    gains = weight_columns(tables, width, outer.shape[0], peers)
    project_down(hidden, outer, gains, outs, steps, ways, width)


def run_experts(gathered, packed, inner_weights, outer_weights):
    ways, _, width = gathered.shape
    peers = len(packed)
    tokens = sum(p.shape[0] for p in packed)
    experts, _, hidden_units, features = inner_weights.shape
    chunk = min(1024, hidden_units)
    work = 2 * tokens * experts * hidden_units * features
    hidden = pl.pallas_call(
        functools.partial(hidden_kernel, chunk),
        out_shape=pltpu.VMEM((experts, hidden_units, tokens), BF16),
        in_specs=[VMEM_SPEC] * 2,
        out_specs=VMEM_SPEC,
        scratch_shapes=[pltpu.VMEM((tokens, features), BF16)],
        compiler_params=limit(6),
        cost_estimate=pl.CostEstimate(
            flops=10**8, bytes_accessed=10**5, transcendentals=0
        ),
        name="hidden",
    )(on_chip(gathered), on_chip(inner_weights))
    operands = (on_chip(hidden), on_chip(outer_weights), *[on_chip(p) for p in packed])

    def down(steps):
        return pl.pallas_call(
            functools.partial(down_kernel, peers, ways, steps),
            out_shape=tuple(
                pltpu.VMEM((tokens, width), F32 if step == 0 else BF16) for step in steps
            ),
            in_specs=[VMEM_SPEC] * len(operands),
            out_specs=(VMEM_SPEC,) * len(steps),
            compiler_params=limit(6),
            cost_estimate=pl.CostEstimate(
                flops=work // 2, bytes_accessed=outer_weights.size, transcendentals=0
            ),
        )(*operands)

    half = max(1, ways // 2)
    far = down(list(range(half, ways)))
    near = down(list(range(half)))
    return [*near, *far]


def state_kernel(
    tokens, seqs, low_rank,
    gathered, act, gate, scan, step_proj, step_bias, decay, skip, attended,
    out, next_state, attended_out,
    square,
):
    attended_out[...] = attended[...]
    ways, rows, _ = gathered.shape
    states = decay.shape[0]
    spans = (rows - tokens) // seqs
    pieces = []
    for span in range(spans):
        piece = None
        for t in range(ways):
            row = tokens + span * seqs
            part = gathered[t, row : row + seqs, :].astype(F32)
            piece = part if piece is None else piece + part
        pieces.append(piece)
    mixing = pieces[0] if spans == 1 else jnp.concatenate(pieces, axis=1)
    square[...] = jnp.zeros_like(square)
    square[:seqs, :] = mixing[:, low_rank : low_rank + LANES]
    columns = square[...].T
    step = (
        jnp.dot(mixing[:, :low_rank].astype(BF16), step_proj[...], preferred_element_type=F32)
        + step_bias[...]
    )
    step_size = jnp.maximum(step, 0.0) + jnp.log1p(jnp.exp(-jnp.abs(step)))
    rates = jnp.exp(decay[...])
    drive = step_size * act[...]
    results = []
    for s in range(seqs):
        in_coef = columns[:states, s : s + 1]
        out_coef = columns[states : 2 * states, s : s + 1]
        new = jnp.exp(-step_size[s : s + 1, :] * rates) * scan[s] + drive[s : s + 1, :] * in_coef
        next_state[s] = new
        results.append(jnp.sum(new * out_coef, axis=0, keepdims=True))
    mixed = jnp.concatenate(results, axis=0) + skip[...] * act[...]
    out[...] = (mixed * silu(gate[...].astype(F32))).astype(BF16)


def update_state(
    gathered, tokens, act, mamba_gate, scan_state, step_proj, step_bias, decay_log, skip_gain,
    attended,
):
    seqs, states, channels = scan_state.shape
    low_rank = step_proj.shape[0]
    block = min(512, channels)
    lane_block = lambda rows: pl.BlockSpec((rows, block), lambda c: (0, c))
    state_block = pl.BlockSpec((seqs, states, block), lambda c: (0, 0, c))
    attended_block = pl.BlockSpec(
        (seqs, attended.shape[1] // (channels // block)), lambda c: (0, c)
    )
    return pl.pallas_call(
        functools.partial(state_kernel, tokens, seqs, low_rank),
        grid=(channels // block,),
        out_shape=(
            jax.ShapeDtypeStruct((seqs, channels), BF16),
            jax.ShapeDtypeStruct(scan_state.shape, F32),
            jax.ShapeDtypeStruct(attended.shape, BF16),
        ),
        in_specs=[
            pl.BlockSpec(gathered.shape, lambda c: (0, 0, 0)),
            lane_block(seqs), lane_block(seqs), state_block,
            lane_block(low_rank), lane_block(1), lane_block(states), lane_block(1),
            attended_block,
        ],
        out_specs=(lane_block(seqs), state_block, attended_block),
        scratch_shapes=[pltpu.VMEM((LANES, LANES), F32)],
        compiler_params=limit(12),
        cost_estimate=pl.CostEstimate(
            flops=3 * 10**9, bytes_accessed=3 * 10**6, transcendentals=0
        ),
        name="state",
    )(
        gathered, act, mamba_gate, scan_state, step_proj,
        step_bias.reshape(1, channels), decay_log, skip_gain.reshape(1, channels),
        on_chip(attended),
    )


def shards(
    mamba_input,
    mamba_gate,
    conv_state,
    scan_state,
    conv_weight,
    conv_bias,
    state_proj,
    step_proj,
    step_bias,
    decay_log,
    skip_gain,
    queries,
    new_entry,
    past_entries,
    lengths,
    expert_input,
    routes,
    slots,
    gates,
    inner_weights,
    outer_weights,
):
    del slots
    peers = lax.axis_size("expert")
    seqs, width = expert_input.shape
    tokens = peers * seqs

    packed = exchange([pack(expert_input, routes, gates)] * peers, "expert")
    act, mix = front(conv_state, mamba_input, conv_weight, conv_bias, state_proj, width)
    mine = join(packed, mix)
    gathered = lax.all_gather(mine, "tensor", axis=0)
    partial = run_experts(gathered, packed, inner_weights, outer_weights)

    arrived = exchange(partial, "tensor")
    attended = attend(queries, new_entry, past_entries, lengths)
    share = arrived[0]
    for part in arrived[1:]:
        share = share + part.astype(F32)
    mamba_out, next_state, attention_out = update_state(
        gathered, tokens, act, mamba_gate, scan_state, step_proj, step_bias, decay_log, skip_gain,
        attended,
    )
    blocks = [share[n * seqs : (n + 1) * seqs] for n in range(peers)]
    blocks = [blocks[0]] + [block.astype(BF16) for block in blocks[1:]]
    returned = exchange(blocks, "expert", back=True)
    merged = returned[0]
    for part in returned[1:]:
        merged = merged + part.astype(F32)
    return (mamba_out, next_state, attention_out, merged.astype(BF16))


def solution(mesh):
    return jax.shard_map(
        shards,
        mesh=mesh,
        in_specs=(
            P(("parts", "expert"), "tensor"),
            P(("parts", "expert"), "tensor"),
            P(("parts", "expert"), None, "tensor"),
            P(("parts", "expert"), None, "tensor"),
            P(None, "tensor"),
            P("tensor"),
            P(None, "tensor"),
            P(None, "tensor"),
            P("tensor"),
            P(None, "tensor"),
            P("tensor"),
            P(("parts", "expert"), "tensor", None),
            P(("parts", "expert"), "tensor", None),
            P(("parts", "expert"), "tensor", None, None),
            P(("parts", "expert")),
            P(("parts", "expert"), "tensor"),
            P(("parts", "expert"), None),
            P(("parts", "expert"), None),
            P(("parts", "expert"), None),
            P("expert", None, "tensor", None),
            P("expert", "tensor", None),
        ),
        out_specs=(
            P(("parts", "expert"), "tensor"),
            P(("parts", "expert"), None, "tensor"),
            P(("parts", "expert"), "tensor"),
            P(("parts", "expert"), "tensor"),
        ),
        check_vma=False,
    )
```
